128 devices in a mesh: blk: 32 (over z, y, x_hi), tp: 4 (over x_lo, core).
Axes of the slice: x: 4 (x_hi: 2, x_lo: 2; x = x_hi * 2 + x_lo), y: 4, z: 4, core: 2. Of those that a mesh axis runs over, the one named last changes fastest.
Arguments:
- tokens: bfloat16 [8192, 2048], P('blk'), may hold values from -27 to 27
- order: int32 [64], replicated, may hold values from 0 to 63, each once
- gain_attn: float32 [2048], replicated, may hold values from 0.1 to 1.9
- gain_ffn: float32 [2048], replicated, may hold values from 0.1 to 1.9
- w_query: bfloat16 [2048, 2048], P(None, 'tp'), may hold values from -3.7565048 to 3.7565048
- w_key: bfloat16 [2048, 512], P(None, 'tp'), may hold values from -0.13258252 to 0.13258252
- w_value: bfloat16 [2048, 512], P(None, 'tp'), may hold values from -0.125 to 0.125
- w_out: bfloat16 [2048, 2048], P('tp'), may hold values from -0.125 to 0.125
- w_gate: bfloat16 [2048, 8192], P(None, 'tp'), may hold values from -0.125 to 0.125
- w_up: bfloat16 [2048, 8192], P(None, 'tp'), may hold values from -0.125 to 0.125
- w_down: bfloat16 [8192, 2048], P('tp'), may hold values from -0.0625 to 0.0625
Outputs:
- layer_out: bfloat16 [8192, 2048], P('blk', 'tp')
The draws below stay inside these ranges and needn't reach their ends.
Inputs may be any that keep to these rules, and one draw needn't show every extreme that they name: `order`: every number 0 to 63 appears once; device b of blk holds stored blocks 2b and 2b + 1.
All inputs are finite; a program needn't handle non-finite values.
Results may differ from the reference program's by a relative error of at most 0.0095.
Values may be sent and summed in bfloat16 or wider, within the bound.
No kernel may reach another device: no remote copies, remote signals or barrier semaphores. Data moves between devices by JAX's collectives and lax.ppermute only.
A program may use at most 128 MiB of HBM per device.

```python
import math
import jax
import jax.numpy as jnp
from jax import lax

D = 2048
QH = 32
KVH = 8
HD = 64
FF = 8192
TOK_DEV = 256
SEQ = 8192
NCHUNK = 64
N_TP = 4


def shared_key_weight(key):
    base = jax.random.normal(jax.random.fold_in(key, 11), (D, KVH * HD), jnp.float32)
    return jnp.clip(base, -6.0, 6.0) * D ** (-0.5)


def draw_w_key(key, part):
    return shared_key_weight(key).astype(jnp.bfloat16)


def draw_w_query(key, part):
    noise = jax.random.normal(jax.random.fold_in(key, 12), (D, QH * HD), jnp.float32)
    noise = jnp.clip(noise, -6.0, 6.0) * (3.0 * D ** (-0.5))
    return noise.astype(jnp.bfloat16)


def draw_tokens(key, part):
    column = jnp.arange(D, dtype=jnp.float32) / (D - 1.0)
    rough = jax.random.uniform(jax.random.fold_in(key, 21), (D,), jnp.float32, 0.7, 1.3)
    col_scale = 0.5 * 4.0 ** column * rough
    base = jnp.clip(jax.random.normal(jax.random.fold_in(key, 24), (SEQ, D), jnp.float32), -6.0, 6.0)
    result = base * col_scale[None, :]
    return result.astype(jnp.bfloat16)


def level_of(rng, extent, shards, smallest, largest):
    factor_of = 1.0
    for dim, shards_of in shards:
        draws = jax.random.uniform(jax.random.fold_in(jax.random.fold_in(rng, 6), dim), (shards_of,), jnp.float32, smallest / len(shards), largest / len(shards))
        factor_of = factor_of * jnp.repeat(jnp.exp(draws), extent[dim] // shards_of).reshape((-1,) + (1,) * (len(extent) - 1 - dim))
    return factor_of


def normal_values(stream_key, shape, deviation, most, pieces=(), held_as=jnp.bfloat16):
    values = jax.random.normal(stream_key, shape, jnp.float32) * deviation
    if len(pieces) > 0:
        values = level_of(stream_key, shape, pieces, -0.22, 0.18) * values
    return jnp.clip(values, min=-most, max=most).astype(held_as)


def setup_inputs(seed: int = 0) -> dict:
    streams_of = jax.random.split(jax.random.key(seed), 12)
    return {
        "tokens": draw_tokens(jax.random.fold_in(streams_of[11], 71), 0),
        "order": jax.random.permutation(streams_of[1], NCHUNK).astype(jnp.int32),
        "gain_attn": jnp.clip(1.0 + 0.18 * jax.random.normal(streams_of[2], (D,), jnp.float32), 0.1, 1.9),
        "gain_ffn": jnp.clip(1.0 + 0.18 * jax.random.normal(streams_of[3], (D,), jnp.float32), 0.1, 1.9),
        "w_query": draw_w_query(jax.random.fold_in(streams_of[11], 71), 0),
        "w_key": draw_w_key(jax.random.fold_in(streams_of[11], 71), 0),
        "w_value": normal_values(streams_of[6], (D, KVH * HD), D ** -0.5, 0.125, ((1, 4),)),
        "w_out": normal_values(streams_of[7], (QH * HD, D), (QH * HD) ** -0.5, 0.125, ((0, 4),)),
        "w_gate": normal_values(streams_of[8], (D, FF), D ** -0.5, 0.125, ((1, 4),)),
        "w_up": normal_values(streams_of[9], (D, FF), D ** -0.5, 0.125, ((1, 4),)),
        "w_down": normal_values(streams_of[10], (FF, D), FF ** -0.5, 0.0625, ((0, 4),)),
    }


EPS = 1e-05
ROPE_BASE = 500000.0
MASKED = -1e+30

def rotate(values, positions):
    half_dim = values.shape[-1] // 2
    freq = ROPE_BASE ** (-(jnp.arange(half_dim, dtype=jnp.float32) * 2.0 / values.shape[-1]))
    angle = positions.astype(jnp.float32)[:, None] * freq[None, :]
    cosine = jnp.cos(angle)[:, None, :]
    sine = jnp.sin(angle)[:, None, :]
    first = values[..., :half_dim]
    second = values[..., half_dim:]
    return jnp.concatenate([first * cosine - second * sine, second * cosine + first * sine], axis=-1)

def reference(tokens, order, gain_attn, gain_ffn, w_query, w_key, w_value, w_out, w_gate, w_up, w_down):
    seq_len = tokens.shape[0]
    half_rows = TOK_DEV // 2
    stored = jnp.arange(seq_len, dtype=jnp.int32)
    position = order[stored // half_rows].astype(jnp.int32) * half_rows + stored % half_rows
    tokens_wide = tokens.astype(jnp.float32)
    normed = (tokens_wide * lax.rsqrt(lax.optimization_barrier(jnp.mean(tokens_wide * tokens_wide, axis=-1, keepdims=True)) + EPS) * gain_attn).astype(jnp.bfloat16)
    queries = jnp.dot(normed, w_query, preferred_element_type=jnp.float32).reshape(seq_len, QH, HD)
    queries = rotate(queries, position).astype(jnp.bfloat16)
    keys = jnp.dot(normed, w_key, preferred_element_type=jnp.float32).reshape(seq_len, KVH, HD)
    keys = rotate(keys, position).astype(jnp.bfloat16)
    values = jnp.dot(normed, w_value, preferred_element_type=jnp.float32).astype(jnp.bfloat16).reshape(seq_len, KVH, HD)
    group = QH // KVH
    query_block = math.gcd(seq_len, 256)
    grouped = queries.reshape(seq_len // query_block, query_block, KVH, group, HD)
    key_wide = keys.astype(jnp.float32)
    value_wide = values.astype(jnp.float32)
    scale = HD ** (-0.5)

    def one_block(inputs):
        block_queries, block_pos = inputs
        scores = jnp.einsum('qkgd,skd->kgqs', block_queries.astype(jnp.float32), key_wide) * scale
        allowed = position[None, :] <= block_pos[:, None]
        scores = jnp.where(allowed, scores, MASKED)
        highest = lax.optimization_barrier(jnp.max(scores, axis=-1, keepdims=True))
        weights = jnp.where(allowed, jnp.exp(scores - highest), 0.0)
        denominator = lax.optimization_barrier(jnp.sum(weights, axis=-1))
        rounded = lax.optimization_barrier(weights.astype(jnp.bfloat16)).astype(jnp.float32)
        mixed = jnp.einsum('kgqs,skd->qkgd', rounded, value_wide)
        return (mixed / jnp.transpose(denominator, (2, 0, 1))[..., None]).astype(jnp.bfloat16)
    heads = lax.map(one_block, (grouped, position.reshape(-1, query_block)))
    heads = heads.reshape(seq_len, QH * HD)
    head_share = QH * HD // N_TP
    attention = jnp.zeros((seq_len, D), jnp.float32)
    for member in range(N_TP):
        lower = member * head_share
        partial_value = jnp.dot(heads[:, lower:lower + head_share], w_out[lower:lower + head_share], preferred_element_type=jnp.float32)
        attention = attention + lax.optimization_barrier(partial_value.astype(jnp.bfloat16)).astype(jnp.float32)
    residual = tokens_wide + attention
    normed_ffn = (residual * lax.rsqrt(lax.optimization_barrier(jnp.mean(residual * residual, axis=-1, keepdims=True)) + EPS) * gain_ffn).astype(jnp.bfloat16)
    gate = jnp.dot(normed_ffn, w_gate, preferred_element_type=jnp.float32)
    up_proj = jnp.dot(normed_ffn, w_up, preferred_element_type=jnp.float32)
    hidden = (jax.nn.silu(gate) * up_proj).astype(jnp.bfloat16)
    unit_share = FF // N_TP
    feed = jnp.zeros((seq_len, D), jnp.float32)
    for member in range(N_TP):
        lower = member * unit_share
        partial_value = jnp.dot(hidden[:, lower:lower + unit_share], w_down[lower:lower + unit_share], preferred_element_type=jnp.float32)
        feed = feed + lax.optimization_barrier(partial_value.astype(jnp.bfloat16)).astype(jnp.float32)
    return (residual + feed).astype(jnp.bfloat16)
```

```python
import functools
import math

import jax
import jax.numpy as jnp
from jax import lax
from jax.experimental import pallas as pl
from jax.experimental.pallas import tpu as pltpu
from jax.sharding import PartitionSpec as P

HD = 64
EPS = 1e-05
ROPE_BASE = 500000.0
NEG = -1e30
HALF = 128
LOG2E = math.log2(math.e)
MIB = 2**20

VM = pl.BlockSpec(memory_space=pltpu.VMEM)
SM = pl.BlockSpec(memory_space=pltpu.SMEM)
ANY = pl.BlockSpec(memory_space=pl.ANY)
BF = jnp.bfloat16
F32 = jnp.float32


def params(mib):
    return pltpu.CompilerParams(vmem_limit_bytes=mib * MIB)


def dot(a, b):
    return jnp.dot(a, b, preferred_element_type=F32)


def rope(u, cos, sin):
    n = u.shape[1] // 128
    outs = []
    lane = lax.broadcasted_iota(jnp.int32, (u.shape[0], 128), 1)
    low = lane % HD < HD // 2
    for k in range(n):
        v = u[:, k * 128 : (k + 1) * 128]
        other = jnp.where(low, pltpu.roll(v, 128 - HD // 2, 1), pltpu.roll(v, HD // 2, 1))
        outs.append(v * cos + other * sin)
    return outs


def kv_kernel(tok_ref, gain_ref, wk_ref, wv_ref, cos_ref, sin_ref, normed_ref, kv_ref):
    rows = 64
    for r in range(0, tok_ref.shape[0], rows):
        x = tok_ref[r : r + rows, :].astype(F32)
        scale = lax.rsqrt(jnp.mean(x * x, axis=-1, keepdims=True) + EPS)
        normed_ref[r : r + rows, :] = (x * scale * gain_ref[...]).astype(BF)
    k = dot(normed_ref[...], wk_ref[...])
    k = rope(k, cos_ref[...], sin_ref[...])[0].astype(BF)
    v = jnp.transpose(dot(normed_ref[...], wv_ref[...])).astype(BF)
    for j in range(2):
        kv_ref[j, :HALF, :] = k[j * HALF : (j + 1) * HALF]
        kv_ref[j, HALF:, :] = v[:, j * HALF : (j + 1) * HALF]


def tile_step(s, adds, i, width, m_old):
    m_new = m_old
    for g, add in enumerate(adds):
        m_new = jnp.maximum(m_new, jnp.max(s[g * 128 : (g + 1) * 128], axis=0, keepdims=True) + add)
    ps = [
        jnp.exp2(s[g * 128 : (g + 1) * 128] + (add - m_new)).astype(BF)
        for g, add in enumerate(adds)
    ]
    return m_new, jnp.concatenate(ps, axis=0)


def accumulate(h, sl, v_blocks, p, m_old, m_new, m_ref, acc_ref):
    vt = jnp.concatenate(v_blocks, axis=1)
    vt = jnp.concatenate([vt, jnp.ones((16, vt.shape[1]), BF)], axis=0)
    pv = dot(vt, p)
    acc_ref[h, :, sl] = acc_ref[h, :, sl] * jnp.exp2(m_old - m_new) + pv
    m_ref[h, :, sl] = m_new


def attend(order_ref, src_ref, first, q_ref, kv_ref, m_ref, acc_ref, me):
    nb = kv_ref.shape[0]
    group = min(8, nb)
    width = 256 if group == 8 else 512
    p0 = order_ref[2 * me]
    p1 = order_ref[2 * me + 1]

    def step(it):
        base = it * group
        pos = [order_ref[src_ref[first + base + g]] for g in range(group)]
        adds = [
            [jnp.where(p < pq, jnp.float32(0.0), jnp.float32(NEG)) for p in pos] for pq in (p0, p1)
        ]
        k_all = jnp.concatenate([kv_ref[base + g, :HALF, :] for g in range(group)], axis=0)

        def rest(h, t, s):
            sl = slice(t * width, (t + 1) * width)
            i = t * width // 512
            m_old = m_ref[h, :, sl]
            m_new, p = tile_step(s, adds[i], i, width, m_old)
            vb = [kv_ref[base + g, HALF + h * HD : HALF + (h + 1) * HD, :] for g in range(group)]
            accumulate(h, sl, vb, p, m_old, m_new, m_ref, acc_ref)

        prev = None
        for h in range(2):
            for t in range(1024 // width):
                s = dot(k_all, q_ref[h, :, t * width : (t + 1) * width])
                if prev is not None:
                    rest(*prev)
                prev = (h, t, s)
        rest(*prev)

    if nb == group:
        step(0)
    else:
        def body(it, c):
            step(it)
            return c
        lax.fori_loop(0, nb // group, body, 0)


def q_kernel(order_ref, me_ref, normed_ref, wq_ref, cos_ref, sin_ref, kv_ref, q_ref, m_ref, acc_ref):
    q = dot(normed_ref[...], wq_ref[...])
    parts = rope(q, cos_ref[...], sin_ref[...])
    q_ref[...] = jnp.zeros(q_ref.shape, BF)
    for k, part in enumerate(parts):
        t = jnp.transpose(part * (HD**-0.5 * LOG2E)).astype(BF)
        for a in range(2):
            head = 2 * k + a
            h, g = head // 4, head % 4
            for i in range(2):
                q_ref[h, h * HD : (h + 1) * HD, i * 512 + g * 128 : i * 512 + (g + 1) * 128] = t[
                    a * HD : (a + 1) * HD, i * HALF : (i + 1) * HALF
                ]
    me = me_ref[0]
    pos = (order_ref[2 * me], order_ref[2 * me + 1])
    key = lax.broadcasted_iota(jnp.int32, (HALF, 512), 0)
    tok = lax.broadcasted_iota(jnp.int32, (HALF, 512), 1) % HALF
    tri = jnp.where(key <= tok, 0.0, NEG).astype(F32)
    k_all = jnp.concatenate([kv_ref[0, :HALF, :], kv_ref[1, :HALF, :]], axis=0)
    for h in range(2):
        for i in range(2):
            sl = slice(i * 512, (i + 1) * 512)
            s = dot(k_all, q_ref[h, :, sl])
            add = jnp.where(pos[1 - i] < pos[i], jnp.float32(0.0), jnp.float32(NEG))
            mine = s[i * HALF : (i + 1) * HALF] + tri
            other = s[(1 - i) * HALF : (2 - i) * HALF]
            m = jnp.maximum(
                jnp.max(mine, axis=0, keepdims=True), jnp.max(other, axis=0, keepdims=True) + add
            )
            pm = jnp.exp2(mine - m).astype(BF)
            po = jnp.exp2(other + (add - m)).astype(BF)
            p = jnp.concatenate([pm, po] if i == 0 else [po, pm], axis=0)
            vt = jnp.concatenate(
                [kv_ref[j, HALF + h * HD : HALF + (h + 1) * HD, :] for j in range(2)], axis=1
            )
            vt = jnp.concatenate([vt, jnp.ones((16, 2 * HALF), BF)], axis=0)
            acc_ref[h, :, sl] = dot(vt, p)
            m_ref[h, :, sl] = m


def chunk_kernel(n, first, order_ref, me_ref, src_ref, q_ref, *refs):
    kvs = refs[:n]
    m_in, acc_in, m_ref, acc_ref = refs[n:]
    m_ref[...] = m_in[...]
    acc_ref[...] = acc_in[...]
    for kv in kvs:
        attend(order_ref, src_ref, first, q_ref, kv, m_ref, acc_ref, me_ref[0])
        first += kv.shape[0]


def last_kernel(n, first, order_ref, me_ref, src_ref, q_ref, *refs):
    kvs = refs[:n]
    m_in, acc_in, wo_hbm, keep_ref, send_ref, m_ref, acc_ref, wo_ref, heads_ref, sem = refs[n:]
    copy = pltpu.make_async_copy(wo_hbm, wo_ref, sem)
    copy.start()
    m_ref[...] = m_in[...]
    acc_ref[...] = acc_in[...]
    for kv in kvs:
        attend(order_ref, src_ref, first, q_ref, kv, m_ref, acc_ref, me_ref[0])
        first += kv.shape[0]
    for i in range(2):
        for k in range(4):
            pair = []
            for a in range(2):
                head = 2 * k + a
                h, g = head // 4, head % 4
                sl = slice(i * 512 + g * 128, i * 512 + (g + 1) * 128)
                pair.append(acc_ref[h, :HD, sl] / acc_ref[h, HD : HD + 1, sl])
            both = jnp.concatenate(pair, axis=0)
            heads_ref[i, :, k * 128 : (k + 1) * 128] = jnp.transpose(both).astype(BF)
    copy.wait()
    core = me_ref[1]
    keep_ref[...] = dot(heads_ref[core], wo_ref[...]).astype(BF)
    send_ref[...] = dot(heads_ref[1 - core], wo_ref[...]).astype(BF)


def ffn_kernel(
    me_ref, tok_ref, own_ref, other_ref, gain_ref, wg_hbm, wu_hbm, wd_hbm,
    resid_ref, keep_ref, send_ref,
    full_ref, normed_ref, acc_ref, wg, wu, wd, sems,
):
    nt = 4
    tf = wg.shape[1] // nt
    copies = []
    for t in range(nt):
        c = slice(t * tf, (t + 1) * tf)
        copies.append(
            [
                pltpu.make_async_copy(wg_hbm.at[:, c], wg.at[:, c], sems.at[0, t]),
                pltpu.make_async_copy(wu_hbm.at[:, c], wu.at[:, c], sems.at[1, t]),
                pltpu.make_async_copy(wd_hbm.at[c, :], wd.at[c, :], sems.at[2, t]),
            ]
        )
    for trio in copies:
        for c in trio:
            c.start()
    core, tp = me_ref[1], me_ref[2]
    rows = 64
    for b in range(2):
        att = (own_ref, other_ref)[b]
        start = pl.multiple_of((core if b == 0 else 1 - core) * HALF, HALF)
        for r in range(0, HALF, rows):
            at = pl.ds(start + r, rows)
            x = tok_ref[at, :].astype(F32) + att[r : r + rows, :].astype(F32)
            full_ref[at, :] = x
            scale = lax.rsqrt(jnp.mean(x * x, axis=-1, keepdims=True) + EPS)
            normed_ref[at, :] = (x * scale * gain_ref[...]).astype(BF)
    share = resid_ref.shape[1]
    resid_ref[...] = full_ref[:, pl.ds(pl.multiple_of(tp * share, share), share)]
    for t in range(nt):
        c = slice(t * tf, (t + 1) * tf)
        copies[t][0].wait()
        gate = dot(normed_ref[...], wg[:, c])
        copies[t][1].wait()
        up = dot(normed_ref[...], wu[:, c])
        hidden = (gate / (1.0 + jnp.exp(-gate)) * up).astype(BF)
        copies[t][2].wait()
        part = dot(hidden, wd[c, :])
        if t == 0:
            acc_ref[...] = part
        else:
            acc_ref[...] += part
    for k in range(2):
        a = pl.ds(pl.multiple_of((2 * k + core) * share, share), share)
        b = pl.ds(pl.multiple_of((2 * k + 1 - core) * share, share), share)
        keep_ref[k, :, :] = acc_ref[:, a]
        send_ref[k, :, :] = acc_ref[:, b].astype(BF)


def sds(shape, dtype=BF):
    return jax.ShapeDtypeStruct(shape, dtype)


def local(tokens, order, gain_attn, gain_ffn, w_query, w_key, w_value, w_out, w_gate, w_up, w_down):
    rows, width = tokens.shape
    me = lax.axis_index("blk").astype(jnp.int32)
    tp = lax.axis_index("tp").astype(jnp.int32)
    core, chip = tp % 2, tp // 2
    meta = jnp.stack([me, core, tp, chip])

    def at(z, y, x):
        return z * 8 + y * 2 + x

    grid = [(z, y, x) for z in range(4) for y in range(4) for x in range(2)]
    xs = [(at(z, y, x), at(z, y, 1 - x)) for z, y, x in grid]

    def zs(k):
        return [(at(z, y, x), at((z + k) % 4, y, x)) for z, y, x in grid]

    def ys(k):
        return [(at(z, y, x), at(z, (y + k) % 4, x)) for z, y, x in grid]

    cores = [(0, 1), (1, 0), (2, 3), (3, 2)]
    chips = [(0, 2), (2, 0), (1, 3), (3, 1)]

    stored = me * rows + jnp.arange(rows, dtype=jnp.int32)
    which = stored // HALF
    match = which[:, None] == jnp.arange(order.shape[0], dtype=jnp.int32)[None, :]
    position = jnp.sum(jnp.where(match, order[None, :], 0), axis=1) * HALF + stored % HALF
    freq = ROPE_BASE ** (-(jnp.arange(HD // 2, dtype=F32) * 2.0 / HD))
    angle = position.astype(F32)[:, None] * jnp.tile(freq, 4)[None, :]
    sign = jnp.where(jnp.arange(128) % HD < HD // 2, -1.0, 1.0).astype(F32)
    cos = jnp.cos(angle)
    sin = jnp.sin(angle) * sign[None, :]

    normed, kv = pl.pallas_call(
        kv_kernel,
        out_shape=[sds((rows, width)), sds((2, 2 * HALF, 128))],
        in_specs=[VM] * 6,
        out_specs=[VM] * 2,
        compiler_params=params(32),
        name="kv",
    )(tokens, gain_attn[None, :], w_key, w_value, cos, sin)

    z, y, x = me // 8, me // 2 % 4, me % 2
    src = []

    def note(half, z, y, x):
        src.append(2 * at(z % 4, y % 4, x) + half)

    kv_x = lax.ppermute(kv, "blk", xs)
    note(0, z, y, 1 - x)
    note(1, z, y, 1 - x)
    q, m, acc = pl.pallas_call(
        q_kernel,
        out_shape=[sds((2, 128, 1024)), sds((2, 1, 1024), F32), sds((2, 80, 1024), F32)],
        in_specs=[SM, SM] + [VM] * 5,
        out_specs=[VM] * 3,
        compiler_params=params(32),
        cost_estimate=pl.CostEstimate(flops=10**9, bytes_accessed=4 * MIB, transcendentals=0),
        name="queries",
    )(order, meta, normed, w_query, cos, sin, kv)
    a2 = jnp.stack([kv[0], kv_x[0]])
    b2 = jnp.stack([kv[1], kv_x[1]])
    steps = (1, 3, 2)
    a_in = [lax.ppermute(a2, "blk", zs(k)) for k in steps]
    b_in = [lax.ppermute(b2, "blk", ys(k)) for k in steps]
    for k in steps:
        note(0, z - k, y, x)
        note(0, z - k, y, 1 - x)
    for k in steps:
        note(1, z, y - k, x)
        note(1, z, y - k, 1 - x)
    a8 = jnp.concatenate([a2] + a_in)
    b8 = jnp.concatenate([b2] + b_in)
    a_far = [lax.ppermute(a8, "blk", ys(k)) for k in steps]
    b_far = [lax.ppermute(b8, "blk", zs(k)) for k in steps]
    for j, k in enumerate(steps):
        for d in (0, *steps):
            note(0, z - d, y - k, x)
            note(0, z - d, y - k, 1 - x)
        for d in (0, *steps):
            note(1, z - k, y - d, x)
            note(1, z - k, y - d, 1 - x)
    src = jnp.stack(src).astype(jnp.int32)

    def chunk(first, kvs, m, acc):
        n = sum(k.shape[0] for k in kvs)
        return pl.pallas_call(
            functools.partial(chunk_kernel, len(kvs), first),
            out_shape=[sds(m.shape, F32), sds(acc.shape, F32)],
            in_specs=[SM] * 3 + [VM] * (3 + len(kvs)),
            out_specs=[VM] * 2,
            compiler_params=params(40),
            cost_estimate=pl.CostEstimate(
                flops=n * 2 * 10**8, bytes_accessed=2 * MIB, transcendentals=0
            ),
            name="chunk",
        )(order, meta, src, q, *kvs, m, acc)

    m, acc = chunk(0, [kv_x], m, acc)
    m, acc = chunk(2, [a8[2:], b8[2:]], m, acc) if False else chunk(2, a_in + b_in, m, acc)
    m, acc = chunk(14, [a_far[0], b_far[0], a_far[1], b_far[1]], m, acc)
    last = [a_far[2], b_far[2]]
    keep, send = pl.pallas_call(
        functools.partial(last_kernel, len(last), 46),
        out_shape=[sds((HALF, width)), sds((HALF, width))],
        in_specs=[SM] * 3 + [VM] * (3 + len(last)) + [ANY],
        out_specs=[VM] * 2,
        scratch_shapes=[
            pltpu.VMEM(m.shape, F32),
            pltpu.VMEM(acc.shape, F32),
            pltpu.VMEM(w_out.shape, BF),
            pltpu.VMEM((2, HALF, w_out.shape[0]), BF),
            pltpu.SemaphoreType.DMA,
        ],
        compiler_params=params(48),
        cost_estimate=pl.CostEstimate(flops=4 * 10**9, bytes_accessed=4 * MIB, transcendentals=0),
        name="last",
    )(order, meta, src, q, *last, m, acc, w_out)

    here = (keep.astype(F32) + lax.ppermute(send, "tp", cores).astype(F32)).astype(BF)
    there = lax.ppermute(here, "tp", chips)
    own = (here.astype(F32) + there.astype(F32)).astype(BF)
    other = lax.ppermute(own, "tp", cores)

    share = width // lax.axis_size("tp")
    resid, keep, send = pl.pallas_call(
        ffn_kernel,
        out_shape=[sds((rows, share), F32), sds((2, rows, share), F32), sds((2, rows, share))],
        in_specs=[SM] + [VM] * 4 + [ANY] * 3,
        out_specs=[VM] * 3,
        scratch_shapes=[
            pltpu.VMEM((rows, width), F32),
            pltpu.VMEM((rows, width), BF),
            pltpu.VMEM((rows, width), F32),
            pltpu.VMEM(w_gate.shape, BF),
            pltpu.VMEM(w_up.shape, BF),
            pltpu.VMEM(w_down.shape, BF),
            pltpu.SemaphoreType.DMA((3, 4)),
        ],
        compiler_params=params(56),
        cost_estimate=pl.CostEstimate(flops=7 * 10**9, bytes_accessed=24 * MIB, transcendentals=0),
        name="ffn",
    )(meta, tokens, own, other, gain_ffn[None, :], w_gate, w_up, w_down)
    both = keep + lax.ppermute(send, "tp", cores).astype(F32)
    mine = lax.dynamic_index_in_dim(both, chip, 0, keepdims=False)
    away = lax.dynamic_index_in_dim(both, 1 - chip, 0, keepdims=False).astype(BF)
    feed = mine + lax.ppermute(away, "tp", chips).astype(F32)
    return (resid + feed).astype(BF)


def solution(mesh):
    placed = (
        P("blk", None),
        P(),
        P(),
        P(),
        P(None, "tp"),
        P(None, "tp"),
        P(None, "tp"),
        P("tp", None),
        P(None, "tp"),
        P(None, "tp"),
        P("tp", None),
    )
    return jax.shard_map(
        local, mesh=mesh, in_specs=placed, out_specs=P("blk", "tp"), check_vma=False
    )
```

```python
import functools
import math

import jax
import jax.numpy as jnp
import numpy as np
from jax import lax
from jax.experimental import pallas as pl
from jax.experimental.pallas import tpu as pltpu
from jax.sharding import PartitionSpec as P


HD = 64
EPS = 1e-05
ROPE_BASE = 500000.0
NEG = -1e30
HIDDEN = -2e30
HALF = 128
LOG2E = math.log2(math.e)
MIB = 2**20

VM = pl.BlockSpec(memory_space=pltpu.VMEM)
SM = pl.BlockSpec(memory_space=pltpu.SMEM)
ANY = pl.BlockSpec(memory_space=pltpu.HBM)
BF = jnp.bfloat16
F32 = jnp.float32


def params(mib):
    return pltpu.CompilerParams(vmem_limit_bytes=mib * MIB)


def dot(a, b):
    return jnp.dot(a, b, preferred_element_type=F32)


def rope(u, cos, sin):
    n = u.shape[1] // 128
    outs = []
    lane = lax.broadcasted_iota(jnp.int32, (u.shape[0], 128), 1)
    low = lane % HD < HD // 2
    for k in range(n):
        v = u[:, k * 128 : (k + 1) * 128]
        other = jnp.where(low, pltpu.roll(v, 128 - HD // 2, 1), pltpu.roll(v, HD // 2, 1))
        outs.append(v * cos + other * sin)
    return outs


def angles():
    freq = ROPE_BASE ** (-(np.arange(HD // 2, dtype=np.float64) * 2.0 / HD))
    freq = np.tile(freq, 4)[None, :]
    near = np.arange(HALF, dtype=np.float64)[:, None] * freq
    far = np.arange(64, dtype=np.float64)[:, None] * HALF * freq
    return np.concatenate([np.cos(near), np.sin(near), np.cos(far), np.sin(far)]).astype(np.float32)


def place():
    me = lax.axis_index("blk").astype(jnp.int32)
    tp = lax.axis_index("tp").astype(jnp.int32)
    return me, tp


def kv_kernel(
    order_ref, tok_hbm, gain_hbm, wk_hbm, wv_hbm, table_hbm,
    normed_ref, mine_ref, send_ref, cos_ref, sin_ref,
    kv_ref, tok_ref, gain_ref, w_ref, table_ref, sems,
):
    rows = 64
    n = tok_ref.shape[0] // rows
    gain_copy = pltpu.make_async_copy(gain_hbm, gain_ref, sems.at[9])
    gain_copy.start()
    copies = []
    for i in range(n):
        part = slice(i * rows, (i + 1) * rows)
        copies.append(pltpu.make_async_copy(tok_hbm.at[part], tok_ref.at[part], sems.at[i]))
    half = w_ref.shape[0] // 2
    for i, a in enumerate((wk_hbm, wv_hbm)):
        b = w_ref.at[:, i * 128 : (i + 1) * 128]
        for part in (slice(0, half), slice(half, 2 * half)):
            copies.append(pltpu.make_async_copy(a.at[part], b.at[part], sems.at[len(copies)]))
    copies.append(pltpu.make_async_copy(table_hbm, table_ref, sems.at[len(copies)]))
    for c in copies:
        c.start()
    me, tp = place()
    core = tp % 2
    gain_copy.wait()
    for r in range(0, n * rows, rows):
        copies[r // rows].wait()
        x = tok_ref[r : r + rows, :].astype(F32)
        scale = lax.rsqrt(jnp.mean(x * x, axis=-1, keepdims=True) + EPS)
        normed_ref[r : r + rows, :] = (x * scale * gain_ref[...]).astype(BF)
    copies[-1].wait()
    lane = lax.broadcasted_iota(jnp.int32, (HALF, 128), 1)
    sign = jnp.where(lane % HD < HD // 2, -1.0, 1.0).astype(F32)
    cos, sin = table_ref[:HALF, :], table_ref[HALF : 2 * HALF, :]
    for j in range(2):
        b = order_ref[2 * me + j]
        cb, sb = table_ref[pl.ds(256 + b, 1), :], table_ref[pl.ds(320 + b, 1), :]
        cos_ref[j * HALF : (j + 1) * HALF, :] = cos * cb - sin * sb
        sin_ref[j * HALF : (j + 1) * HALF, :] = (sin * cb + cos * sb) * sign
    for i in range(4):
        copies[n + i].wait()
    both = dot(normed_ref[...], w_ref[...])
    k = rope(both[:, :128], cos_ref[...], sin_ref[...])[0].astype(BF)
    v = jnp.transpose(both[:, 128:]).astype(BF)
    for j in range(2):
        kv_ref[j, :HALF, :] = k[j * HALF : (j + 1) * HALF]
        kv_ref[j, HALF:, :] = v[:, j * HALF : (j + 1) * HALF]
    mine_ref[...] = kv_ref[core]
    send_ref[...] = kv_ref[1 - core]


def pack_kernel(*refs):
    out = refs[-1]
    at = 0
    for r in refs[:-1]:
        out[at : at + r.shape[0]] = r[...]
        at += r.shape[0]


def q_kernel(normed_ref, wq_hbm, cos_ref, sin_ref, q_ref, wq_ref, sem):
    part = wq_ref.shape[0] // 4
    copies = []
    for i in range(4):
        at = slice(i * part, (i + 1) * part)
        copies.append(pltpu.make_async_copy(wq_hbm.at[at], wq_ref.at[at], sem.at[i]))
    for c in copies:
        c.start()
    for c in copies:
        c.wait()
    q = dot(normed_ref[...], wq_ref[...])
    parts = rope(q, cos_ref[...], sin_ref[...])
    q_ref[...] = jnp.zeros(q_ref.shape, BF)
    for k, part in enumerate(parts):
        t = jnp.transpose(part * (HD**-0.5 * LOG2E)).astype(BF)
        for a in range(2):
            head = 2 * k + a
            h, g = head // 4, head % 4
            for i in range(2):
                q_ref[h, h * HD : (h + 1) * HD, i * 512 + g * 128 : i * 512 + (g + 1) * 128] = t[
                    a * HD : (a + 1) * HD, i * HALF : (i + 1) * HALF
                ]


def attend(order_ref, src_ref, first, own, q_refs, kv_ref, m_ref, acc_ref):
    me, tp = place()
    core = tp % 2
    width = 256
    group = kv_ref.shape[0]
    pq = [order_ref[2 * me + i] for i in range(2)]
    pos = [order_ref[src_ref[first + g]] for g in range(group)]
    adds = [[jnp.where(p < q, jnp.float32(0.0), jnp.float32(HIDDEN)) for p in pos] for q in pq]
    if own:
        key = lax.broadcasted_iota(jnp.int32, (HALF, width), 0)
        tok = lax.broadcasted_iota(jnp.int32, (HALF, width), 1) % HALF
        tri = jnp.where(key <= tok, 0.0, HIDDEN).astype(F32)

    def pair(p):
        q_ref = q_refs[p]
        k_all = jnp.concatenate([kv_ref[g, p, :HALF, :] for g in range(group)], axis=0)

        def rest(h, t, s):
            sl = slice(t * width, (t + 1) * width)
            i = t * width // 512
            add = adds[i]
            parts = [s[g * HALF : (g + 1) * HALF] for g in range(group)]
            if own:
                parts[0] = parts[0] + jnp.where(core == i, tri, add[0])
                add = [jnp.float32(0.0), *add[1:]]
            m_old = jnp.full((1, width), NEG, F32) if own else m_ref[2 * p + h, :, sl]
            m_new = m_old
            for x, b in zip(parts, add):
                m_new = jnp.maximum(m_new, jnp.max(x, axis=0, keepdims=True) + b)
            e = [jnp.exp2(x + (b - m_new)).astype(BF) for x, b in zip(parts, add)]
            vt = [kv_ref[g, p, HALF + h * HD : HALF + (h + 1) * HD, :] for g in range(group)]
            vt = jnp.concatenate(vt, axis=1)
            vt = jnp.concatenate([vt, jnp.ones((16, vt.shape[1]), BF)], axis=0)
            new = dot(vt, jnp.concatenate(e, axis=0))
            if not own:
                new = acc_ref[2 * p + h, :, sl] * jnp.exp2(m_old - m_new) + new
            acc_ref[2 * p + h, :, sl] = new
            m_ref[2 * p + h, :, sl] = m_new

        prev = None
        for h in range(2):
            for t in range(1024 // width):
                s = dot(k_all, q_ref[h, :, t * width : (t + 1) * width])
                if prev is not None:
                    rest(*prev)
                prev = (h, t, s)
        rest(*prev)

    for p in range(2):
        pair(p)


def start_kernel(order_ref, src_ref, q_ref, q2_ref, kv_ref, m_ref, acc_ref):
    attend(order_ref, src_ref, 0, True, (q_ref, q2_ref), kv_ref, m_ref, acc_ref)


def next_kernel(first, order_ref, src_ref, q_ref, q2_ref, kv_ref, m_in, acc_in, m_ref, acc_ref):
    m_ref[...] = m_in[...]
    acc_ref[...] = acc_in[...]
    attend(order_ref, src_ref, first, False, (q_ref, q2_ref), kv_ref, m_ref, acc_ref)


def last_kernel(
    first, order_ref, src_ref, q_ref, q2_ref, kv_ref, m_in, acc_in, keep_ref, send_ref, m_ref, acc_ref
):
    m_ref[...] = m_in[...]
    acc_ref[...] = acc_in[...]
    attend(order_ref, src_ref, first, False, (q_ref, q2_ref), kv_ref, m_ref, acc_ref)
    core = place()[1] % 2
    for ref, i in ((keep_ref, core), (send_ref, 1 - core)):
        at = pl.ds(pl.multiple_of(i * 512, 512), 512)
        for j in range(4):
            ref[j, :72, :] = acc_ref[j, :72, at]
            ref[j, 72:, :] = jnp.broadcast_to(m_ref[j, :, at], (8, 512))


def project_kernel(mine_ref, got_ref, wo_ref, wo2_ref, out_ref, heads_ref):
    for p in range(2):
        for h in range(2):
            a, b = 2 * p + h, 2 * (1 - p) + h
            ma, mb = mine_ref[a, 72:73, :], got_ref[b, 72:73, :]
            m = jnp.maximum(ma, mb)
            fa, fb = jnp.exp2(ma - m), jnp.exp2(mb - m)
            low = mine_ref[a, HD : HD + 1, :] * fa + got_ref[b, HD : HD + 1, :] * fb
            value = (mine_ref[a, :HD, :] * fa + got_ref[b, :HD, :] * fb) / low
            for k in range(2):
                both = jnp.concatenate(
                    [value[:, (2 * k + g) * 128 : (2 * k + g + 1) * 128] for g in range(2)], axis=0
                )
                col = (p * 4 + h * 2 + k) * 128
                heads_ref[:, col : col + 128] = jnp.transpose(both).astype(BF)
    half = wo_ref.shape[0]
    out = dot(heads_ref[:, :half], wo_ref[...]) + dot(heads_ref[:, half:], wo2_ref[...])
    out_ref[...] = out.astype(BF)


def fetch_kernel(*refs):
    n = (len(refs) - 1) // 2
    parts = 8
    copies = []
    for i in range(n):
        a, b = refs[i], refs[n + i]
        rows = a.shape[0] // parts
        for j in range(parts):
            at = slice(j * rows, (j + 1) * rows)
            copies.append(pltpu.make_async_copy(a.at[at], b.at[at], refs[-1].at[i, j]))
    for c in copies:
        c.start()
    for c in copies:
        c.wait()


def ffn_kernel(
    tok_ref, own_ref, other_ref, gain_ref, wg, wu, wd,
    resid_ref, keep_ref, send_ref,
    full_ref, normed_ref, acc_ref,
):
    nt = 4
    tf = wg.shape[1] // nt
    tp = place()[1]
    core = tp % 2
    rows = 64
    for b in range(2):
        att = (own_ref, other_ref)[b]
        start = pl.multiple_of((core if b == 0 else 1 - core) * HALF, HALF)
        for r in range(0, HALF, rows):
            at = pl.ds(start + r, rows)
            x = tok_ref[at, :].astype(F32) + att[r : r + rows, :].astype(F32)
            full_ref[at, :] = x
            scale = lax.rsqrt(jnp.mean(x * x, axis=-1, keepdims=True) + EPS)
            normed_ref[at, :] = (x * scale * gain_ref[...]).astype(BF)
    share = resid_ref.shape[1]
    resid_ref[...] = full_ref[:, pl.ds(pl.multiple_of(tp * share, share), share)]
    acc_ref[...] = jnp.zeros(acc_ref.shape, F32)

    def body(t, carry):
        c = pl.ds(pl.multiple_of(t * tf, tf), tf)
        gate = dot(normed_ref[...], wg[:, c])
        up = dot(normed_ref[...], wu[:, c])
        hidden = (gate / (1.0 + jnp.exp(-gate)) * up).astype(BF)
        acc_ref[...] += dot(hidden, wd[c, :])
        return carry

    lax.fori_loop(0, nt, body, 0)
    for k in range(2):
        a = pl.ds(pl.multiple_of((2 * k + core) * share, share), share)
        b = pl.ds(pl.multiple_of((2 * k + 1 - core) * share, share), share)
        keep_ref[k, :, :] = acc_ref[:, a]
        send_ref[k, :, :] = acc_ref[:, b].astype(BF)


def sum_kernel(a_ref, b_ref, out_ref):
    out_ref[...] = (a_ref[...].astype(F32) + b_ref[...].astype(F32)).astype(BF)


def sds(shape, dtype=BF):
    return jax.ShapeDtypeStruct(shape, dtype)


def index_of(z, y, x):
    return z % 4 * 8 + y % 4 * 2 + x


GRID = [(z, y, x) for z in range(4) for y in range(4) for x in range(2)]
STEPS = (1, 3, 2)
BACK = (3, 1, 2)
FLIP_X = [(index_of(z, y, x), index_of(z, y, 1 - x)) for z, y, x in GRID]
CORES = [(0, 1), (1, 0), (2, 3), (3, 2)]
CHIPS = [(0, 2), (2, 0), (1, 3), (3, 1)]


def along(second, k):
    out = []
    for z, y, x in GRID:
        for tp in range(4):
            if (tp % 2 == 0) != second:
                to = index_of(z + k, y, x)
            else:
                to = index_of(z, y + k, x)
            out.append((index_of(z, y, x) * 4 + tp, to * 4 + tp))
    return out


def arrivals(z, y, x, core):
    out = []
    for k in (0, *BACK):
        for d in (0, *STEPS):
            dz, dy = (d, k) if core == 0 else (k, d)
            for xx in (x, 1 - x):
                out.append(2 * index_of(z - dz, y - dy, xx) + core)
    return out


def stay(x):
    return pltpu.with_memory_space_constraint(x, pltpu.HBM)


def call(kernel, out, ins, outs, args, scratch=(), mib=56, flops=10**7, nbytes=MIB):
    return pl.pallas_call(
        kernel,
        out_shape=out,
        in_specs=ins,
        out_specs=outs,
        scratch_shapes=scratch,
        compiler_params=params(mib),
        cost_estimate=pl.CostEstimate(flops=flops, bytes_accessed=nbytes, transcendentals=0),
    )(*args)


def layer(tokens, order, gain_attn, gain_ffn, w_query, w_key, w_value, w_out, w_gate, w_up, w_down):
    rows, width = tokens.shape
    me, tp = place()
    chip = tp // 2
    every = ("blk", "tp")
    order = stay(order)
    table = jnp.asarray(angles())
    src = jnp.asarray(np.array([arrivals(*g, c) for g in GRID for c in range(2)], np.int32))
    src = lax.dynamic_slice_in_dim(src, 2 * me + tp % 2, 1, 0)[0]
    trig = sds((rows, 128), F32)
    half = sds((2 * HALF, 128))
    dma = pltpu.SemaphoreType.DMA

    normed, mine, send, cos, sin = call(
        kv_kernel,
        [sds((rows, width)), half, half, trig, trig],
        [SM, ANY, ANY, ANY, ANY, ANY], [VM] * 5,
        (order, stay(tokens), stay(gain_attn[None, :]), stay(w_key), stay(w_value), stay(table)),
        [
            pltpu.VMEM((2, 2 * HALF, 128), BF),
            pltpu.VMEM(tokens.shape, BF),
            pltpu.VMEM((1, width), F32),
            pltpu.VMEM((width, 256), BF),
            pltpu.VMEM(table.shape, F32),
            dma((10,)),
        ],
        mib=14,
    )
    got = lax.ppermute(send, "tp", CORES)
    one = call(pack_kernel, sds((2, 2 * HALF, 128)), [VM] * 2, VM, (mine[None], got[None]), mib=4)
    other = lax.ppermute(one, "blk", FLIP_X)
    two = call(
        pack_kernel, sds((2, 2, 2 * HALF, 128)), [VM] * 2, VM, (one[None], other[None]), mib=4
    )
    near = [lax.ppermute(two, every, along(False, k)) for k in STEPS]
    eight = call(pack_kernel, sds((8, 2, 2 * HALF, 128)), [VM] * 4, VM, (two, *near), mib=8)
    q = call(
        q_kernel, sds((2, 128, 1024)),
        [VM, ANY, VM, VM], VM,
        (normed, w_query, cos, sin),
        [pltpu.VMEM(w_query.shape, BF), dma((4,))],
        mib=16, flops=10**9, nbytes=4 * MIB,
    )
    q2 = lax.ppermute(q, "tp", CORES)
    wo2 = lax.ppermute(w_out, "tp", CORES)
    far = [lax.ppermute(eight, every, along(True, k)) for k in BACK[:2]]
    far.append(lax.ppermute(far[0], every, along(True, 3)))

    state = [sds((4, 1, 1024), F32), sds((4, 80, 1024), F32)]
    m, acc = call(
        start_kernel, state, [SM] * 2 + [VM] * 3, [VM] * 2, (order, src, q, q2, eight),
        mib=16, flops=2 * 10**9, nbytes=2 * MIB,
    )
    for j in range(2):
        m, acc = call(
            functools.partial(next_kernel, 8 * (j + 1)), state,
            [SM] * 2 + [VM] * 5, [VM] * 2, (order, src, q, q2, far[j], m, acc),
            mib=16, flops=2 * 10**9, nbytes=2 * MIB,
        )
    keep, send = call(
        functools.partial(last_kernel, 24), [sds((4, 80, 512), F32)] * 2,
        [SM] * 2 + [VM] * 5, [VM] * 2, (order, src, q, q2, far[2], m, acc),
        [pltpu.VMEM(s.shape, F32) for s in state],
        mib=16, flops=2 * 10**9, nbytes=2 * MIB,
    )
    got = lax.ppermute(send, "tp", CORES)
    here = call(
        project_kernel, sds((HALF, width)), [VM] * 4, VM, (keep, got, w_out, wo2),
        [pltpu.VMEM((HALF, 2 * w_out.shape[0]), BF)],
        mib=16, flops=10**9, nbytes=4 * MIB,
    )
    there = lax.ppermute(here, "tp", CHIPS)
    weights = (w_gate, w_up, w_down)
    weights = call(
        fetch_kernel, [sds(w.shape) for w in weights], [ANY] * 3, [VM] * 3,
        tuple(stay(w) for w in weights), [dma((3, 8))], mib=2, nbytes=24 * MIB,
    )
    weights = [pltpu.with_memory_space_constraint(w, pltpu.VMEM) for w in weights]
    own = call(sum_kernel, sds((HALF, width)), [VM] * 2, VM, (here, there), mib=4)
    other = lax.ppermute(own, "tp", CORES)

    share = width // lax.axis_size("tp")
    resid, keep, send = call(
        ffn_kernel,
        [sds((rows, share), F32), sds((2, rows, share), F32), sds((2, rows, share))],
        [VM] * 7, [VM] * 3,
        (tokens, own, other, gain_ffn[None, :], *weights),
        [
            pltpu.VMEM((rows, width), F32),
            pltpu.VMEM((rows, width), BF),
            pltpu.VMEM((rows, width), F32),
        ],
        mib=16, flops=7 * 10**9, nbytes=24 * MIB,
    )
    both = keep + lax.ppermute(send, "tp", CORES).astype(F32)
    mine = lax.dynamic_index_in_dim(both, chip, 0, keepdims=False)
    away = lax.dynamic_index_in_dim(both, 1 - chip, 0, keepdims=False).astype(BF)
    feed = mine + lax.ppermute(away, "tp", CHIPS).astype(F32)
    return (resid + feed).astype(BF)


def solution(mesh):
    placed = (
        P("blk", None),
        P(),
        P(),
        P(),
        P(None, "tp"),
        P(None, "tp"),
        P(None, "tp"),
        P("tp", None),
        P(None, "tp"),
        P(None, "tp"),
        P("tp", None),
    )
    return jax.shard_map(
        layer, mesh=mesh, in_specs=placed, out_specs=P("blk", "tp"), check_vma=False
    )
```

```python
import functools
import math

import jax
import jax.numpy as jnp
import numpy as np
from jax import lax
from jax.experimental import pallas as pl
from jax.experimental.pallas import tpu as pltpu
from jax.sharding import PartitionSpec as P


HD = 64
EPS = 1e-05
ROPE_BASE = 500000.0
COLUMNS = (0, 1, 3, 2)
NEG = -1e30
HIDDEN = -2e30
HALF = 128
LOG2E = math.log2(math.e)
MIB = 2**20

VM = pl.BlockSpec(memory_space=pltpu.VMEM)
SM = pl.BlockSpec(memory_space=pltpu.SMEM)
ANY = pl.BlockSpec(memory_space=pltpu.HBM)
BF = jnp.bfloat16
F32 = jnp.float32


def params(mib):
    return pltpu.CompilerParams(vmem_limit_bytes=mib * MIB)


def dot(a, b):
    return jnp.dot(a, b, preferred_element_type=F32)


def rope(u, cos, sin):
    n = u.shape[1] // 128
    outs = []
    lane = lax.broadcasted_iota(jnp.int32, (u.shape[0], 128), 1)
    low = lane % HD < HD // 2
    for k in range(n):
        v = u[:, k * 128 : (k + 1) * 128]
        other = jnp.where(low, pltpu.roll(v, 128 - HD // 2, 1), pltpu.roll(v, HD // 2, 1))
        outs.append(v * cos + other * sin)
    return outs


def angles():
    freq = ROPE_BASE ** (-(np.arange(HD // 2, dtype=np.float64) * 2.0 / HD))
    freq = np.tile(freq, 4)[None, :]
    near = np.arange(HALF, dtype=np.float64)[:, None] * freq
    far = np.arange(64, dtype=np.float64)[:, None] * HALF * freq
    return np.concatenate([np.cos(near), np.sin(near), np.cos(far), np.sin(far)]).astype(np.float32)


def place():
    me = lax.axis_index("blk").astype(jnp.int32)
    tp = lax.axis_index("tp").astype(jnp.int32)
    return me, tp


def kv_kernel(
    order_ref, tok_hbm, gain_hbm, wk_hbm, wv_hbm, table_hbm,
    normed_ref, mine_ref, send_ref, cos_ref, sin_ref,
    kv_ref, tok_ref, gain_ref, w_ref, table_ref, sems,
):
    rows = 64
    n = tok_ref.shape[0] // rows
    gain_copy = pltpu.make_async_copy(gain_hbm, gain_ref, sems.at[9])
    gain_copy.start()
    copies = []
    for i in range(n):
        part = slice(i * rows, (i + 1) * rows)
        copies.append(pltpu.make_async_copy(tok_hbm.at[part], tok_ref.at[part], sems.at[i]))
    half = w_ref.shape[0] // 2
    for i, a in enumerate((wk_hbm, wv_hbm)):
        b = w_ref.at[:, i * 128 : (i + 1) * 128]
        for part in (slice(0, half), slice(half, 2 * half)):
            copies.append(pltpu.make_async_copy(a.at[part], b.at[part], sems.at[len(copies)]))
    copies.append(pltpu.make_async_copy(table_hbm, table_ref, sems.at[len(copies)]))
    for c in copies:
        c.start()
    me, tp = place()
    core = tp % 2
    gain_copy.wait()
    for r in range(0, n * rows, rows):
        copies[r // rows].wait()
        x = tok_ref[r : r + rows, :].astype(F32)
        scale = lax.rsqrt(jnp.mean(x * x, axis=-1, keepdims=True) + EPS)
        normed_ref[r : r + rows, :] = (x * scale * gain_ref[...]).astype(BF)
    copies[-1].wait()
    lane = lax.broadcasted_iota(jnp.int32, (HALF, 128), 1)
    sign = jnp.where(lane % HD < HD // 2, -1.0, 1.0).astype(F32)
    cos, sin = table_ref[:HALF, :], table_ref[HALF : 2 * HALF, :]
    for j in range(2):
        b = order_ref[2 * me + j]
        cb, sb = table_ref[pl.ds(256 + b, 1), :], table_ref[pl.ds(320 + b, 1), :]
        cos_ref[j * HALF : (j + 1) * HALF, :] = cos * cb - sin * sb
        sin_ref[j * HALF : (j + 1) * HALF, :] = (sin * cb + cos * sb) * sign
    for i in range(4):
        copies[n + i].wait()
    both = dot(normed_ref[...], w_ref[...])
    k = rope(both[:, :128], cos_ref[...], sin_ref[...])[0].astype(BF)
    v = jnp.transpose(both[:, 128:]).astype(BF)
    for j in range(2):
        kv_ref[j, :HALF, :] = k[j * HALF : (j + 1) * HALF]
        kv_ref[j, HALF:, :] = v[:, j * HALF : (j + 1) * HALF]
    mine_ref[...] = kv_ref[core]
    send_ref[...] = kv_ref[1 - core]


def pack_kernel(*refs):
    out = refs[-1]
    at = 0
    for r in refs[:-1]:
        out[at : at + r.shape[0]] = r[...]
        at += r.shape[0]


def q_kernel(normed_ref, wq_hbm, cos_ref, sin_ref, q_ref, wq_ref, sem):
    part = wq_ref.shape[0] // 4
    copies = []
    for i in range(4):
        at = slice(i * part, (i + 1) * part)
        copies.append(pltpu.make_async_copy(wq_hbm.at[at], wq_ref.at[at], sem.at[i]))
    for c in copies:
        c.start()
    for c in copies:
        c.wait()
    q = dot(normed_ref[...], wq_ref[...])
    parts = rope(q, cos_ref[...], sin_ref[...])
    q_ref[...] = jnp.zeros(q_ref.shape, BF)
    for k, part in enumerate(parts):
        t = jnp.transpose(part * (HD**-0.5 * LOG2E)).astype(BF)
        for a in range(2):
            head = 2 * k + a
            h, g = head // 4, head % 4
            for i in range(2):
                q_ref[h, h * HD : (h + 1) * HD, i * 512 + g * 128 : i * 512 + (g + 1) * 128] = t[
                    a * HD : (a + 1) * HD, i * HALF : (i + 1) * HALF
                ]


def attend(order_ref, blocks, own, q_refs, m_ref, acc_ref):
    me, tp = place()
    core = tp % 2
    width = 256
    pq = [order_ref[2 * me + i] for i in range(2)]
    z, y, x = me // 8, me // 2 % 4, me % 2
    pos = []
    for _, _, d, k, flip in blocks:
        zz = (z + 4 - jnp.where(core == 0, d, k)) % 4
        yy = (y + 4 - jnp.where(core == 0, k, d)) % 4
        xx = 1 - x if flip else x
        pos.append(order_ref[2 * (zz * 8 + yy * 2 + xx) + core])
    adds = [[jnp.where(p < q, jnp.float32(0.0), jnp.float32(HIDDEN)) for p in pos] for q in pq]
    if own:
        key = lax.broadcasted_iota(jnp.int32, (HALF, width), 0)
        tok = lax.broadcasted_iota(jnp.int32, (HALF, width), 1) % HALF
        tri = jnp.where(key <= tok, 0.0, HIDDEN).astype(F32)

    def scores(p, h, t):
        keys = jnp.concatenate([r[g, p, :HALF, :] for r, g, _, _, _ in blocks], axis=0)
        return dot(keys, q_refs[p][h, :, t * width : (t + 1) * width])

    def rest(p, h, t, s):
        sl = slice(t * width, (t + 1) * width)
        i = t * width // 512
        add = adds[i]
        parts = [s[g * HALF : (g + 1) * HALF] for g in range(len(blocks))]
        if own:
            parts[0] = parts[0] + jnp.where(core == i, tri, add[0])
            add = [jnp.float32(0.0), *add[1:]]
        m_old = jnp.full((1, width), NEG, F32) if own else m_ref[2 * p + h, :, sl]
        m_new = m_old
        for v, b in zip(parts, add):
            m_new = jnp.maximum(m_new, jnp.max(v, axis=0, keepdims=True) + b)
        e = [jnp.exp2(v + (b - m_new)).astype(BF) for v, b in zip(parts, add)]
        vt = [r[g, p, HALF + h * HD : HALF + (h + 1) * HD, :] for r, g, _, _, _ in blocks]
        vt = jnp.concatenate(vt, axis=1)
        vt = jnp.concatenate([vt, jnp.ones((16, vt.shape[1]), BF)], axis=0)
        new = dot(vt, jnp.concatenate(e, axis=0))
        if not own:
            new = acc_ref[2 * p + h, :, sl] * jnp.exp2(m_old - m_new) + new
        acc_ref[2 * p + h, :, sl] = new
        m_ref[2 * p + h, :, sl] = m_new

    waiting = []
    for p in range(2):
        for h in range(2):
            for t in range(1024 // width):
                waiting.append((p, h, t, scores(p, h, t)))
                if len(waiting) > 3:
                    rest(*waiting.pop(0))
    for w in waiting:
        rest(*w)


def all_of(ref, columns, k):
    return [(ref, 2 * i + f, d, k, f == 1) for i, d in enumerate(columns) for f in range(2)]


def start_kernel(order_ref, q_ref, q2_ref, kv_ref, m_ref, acc_ref):
    attend(order_ref, all_of(kv_ref, COLUMNS, 0), True, (q_ref, q2_ref), m_ref, acc_ref)


def next_kernel(step, order_ref, q_ref, q2_ref, kv_ref, m_in, acc_in, m_ref, acc_ref):
    m_ref[...] = m_in[...]
    acc_ref[...] = acc_in[...]
    attend(order_ref, all_of(kv_ref, COLUMNS, step), False, (q_ref, q2_ref), m_ref, acc_ref)


def last_kernel(
    step, order_ref, q_ref, q2_ref, kv_ref, m_in, acc_in, keep_ref, send_ref, m_ref, acc_ref
):
    m_ref[...] = m_in[...]
    acc_ref[...] = acc_in[...]
    attend(order_ref, all_of(kv_ref, COLUMNS, step), False, (q_ref, q2_ref), m_ref, acc_ref)
    core = place()[1] % 2
    for ref, i in ((keep_ref, core), (send_ref, 1 - core)):
        at = pl.ds(pl.multiple_of(i * 512, 512), 512)
        for j in range(4):
            ref[j, :72, :] = acc_ref[j, :72, at]
            ref[j, 72:, :] = jnp.broadcast_to(m_ref[j, :, at], (8, 512))


def join_kernel(mine_ref, got_ref, heads_ref):
    for p in range(2):
        for h in range(2):
            a, b = 2 * p + h, 2 * (1 - p) + h
            ma, mb = mine_ref[a, 72:73, :], got_ref[b, 72:73, :]
            m = jnp.maximum(ma, mb)
            fa, fb = jnp.exp2(ma - m), jnp.exp2(mb - m)
            low = mine_ref[a, HD : HD + 1, :] * fa + got_ref[b, HD : HD + 1, :] * fb
            value = (mine_ref[a, :HD, :] * fa + got_ref[b, :HD, :] * fb) / low
            for k in range(2):
                both = jnp.concatenate(
                    [value[:, (2 * k + g) * 128 : (2 * k + g + 1) * 128] for g in range(2)], axis=0
                )
                col = (p * 4 + h * 2 + k) * 128
                heads_ref[:, col : col + 128] = jnp.transpose(both).astype(BF)


def project_kernel(heads_ref, wo_ref, wo2_ref, out_ref):
    half = wo_ref.shape[0]
    out_ref[...] = dot(heads_ref[:, :half], wo_ref[...]) + dot(heads_ref[:, half:], wo2_ref[...])


def rows_of(i):
    return pl.ds(pl.multiple_of(i * HALF, HALF), HALF)


def normalize(x, gain_ref):
    scale = lax.rsqrt(jnp.mean(x * x, axis=-1, keepdims=True) + EPS)
    return (x * scale * gain_ref[...]).astype(BF)


def residual_rows(tok_ref, att_ref, gain_ref, block, normed_ref, resid_ref, full_ref):
    rows = 64
    start = pl.multiple_of(block * HALF, HALF)
    for r in range(0, HALF, rows):
        x = tok_ref[pl.ds(start + r, rows), :].astype(F32) + att_ref[r : r + rows, :].astype(F32)
        full_ref[r : r + rows, :] = x
        normed_ref[r : r + rows, :] = normalize(x, gain_ref)
    share = resid_ref.shape[1]
    tp = place()[1]
    resid_ref[...] = full_ref[:, pl.ds(pl.multiple_of(tp * share, share), share)]


def own_kernel(
    part_ref, heads_ref, wo_ref, wo2_ref, tok_ref, gain_ref, att_ref, normed_ref, resid_ref, full_ref
):
    half = wo_ref.shape[0]
    att = part_ref[...] + dot(heads_ref[:, :half], wo_ref[...])
    att_ref[...] = (att + dot(heads_ref[:, half:], wo2_ref[...])).astype(BF)
    core = place()[1] % 2
    residual_rows(tok_ref, att_ref, gain_ref, core, normed_ref, resid_ref, full_ref)


def gated(normed, wg, wu, store):
    tf = 512

    def body(t, carry):
        c = pl.ds(pl.multiple_of(t * tf, tf), tf)
        gate = dot(normed[...], wg[:, c])
        up = dot(normed[...], wu[:, c])
        store(c, (gate / (1.0 + jnp.exp(-gate)) * up).astype(BF))
        return carry

    lax.fori_loop(0, wg.shape[1] // tf, body, 0)


def hidden_kernel(normed_ref, wg, wu, hidden_ref):
    def store(c, value):
        hidden_ref[:, c] = value

    gated(normed_ref, wg, wu, store)


def down_slice(hidden_ref, wd, i):
    return dot(hidden_ref[...], wd[:, pl.ds(pl.multiple_of(i * 512, 512), 512)])


def away_kernel(
    tok_ref, att_ref, gain_ref, mine_ref, wg, wu, wd,
    resid_ref, hidden_ref, keep_ref, send_ref,
    normed_ref, full_ref,
):
    tp = place()[1]
    core, chip = tp % 2, tp // 2
    residual_rows(tok_ref, att_ref, gain_ref, 1 - core, normed_ref, resid_ref, full_ref)
    hidden_ref[rows_of(core), :] = mine_ref[...]

    def store(c, value):
        hidden_ref[rows_of(1 - core), c] = value

    gated(normed_ref, wg, wu, store)
    keep_ref[...] = down_slice(hidden_ref, wd, 2 * (1 - chip) + core)
    send_ref[...] = down_slice(hidden_ref, wd, 2 * (1 - chip) + 1 - core).astype(BF)


def home_kernel(hidden_ref, wd, own_ref, other_ref, keep_ref, send_ref):
    tp = place()[1]
    core, chip = tp % 2, tp // 2
    part = down_slice(hidden_ref, wd, 2 * chip + core)
    keep_ref[...] = part
    for i, ref in ((core, own_ref), (1 - core, other_ref)):
        keep_ref[rows_of(i), :] += ref[...]
    send_ref[...] = down_slice(hidden_ref, wd, 2 * chip + 1 - core).astype(BF)


def final_kernel(keep_ref, a_ref, b_ref, out_ref):
    out_ref[...] = (keep_ref[...] + a_ref[...].astype(F32) + b_ref[...].astype(F32)).astype(BF)


def sum_kernel(a_ref, b_ref, out_ref):
    out_ref[...] = (a_ref[...].astype(F32) + b_ref[...].astype(F32)).astype(BF)


def sds(shape, dtype=BF):
    return jax.ShapeDtypeStruct(shape, dtype)


def index_of(z, y, x):
    return z % 4 * 8 + y % 4 * 2 + x


GRID = [(z, y, x) for z in range(4) for y in range(4) for x in range(2)]
STEPS = (1, 3, 2)
BACK = (3, 1, 2)
FLIP_X = [(index_of(z, y, x), index_of(z, y, 1 - x)) for z, y, x in GRID]
CORES = [(0, 1), (1, 0), (2, 3), (3, 2)]
CHIPS = [(0, 2), (2, 0), (1, 3), (3, 1)]


def along(second, k):
    out = []
    for z, y, x in GRID:
        for tp in range(4):
            if (tp % 2 == 0) != second:
                to = index_of(z + k, y, x)
            else:
                to = index_of(z, y + k, x)
            out.append((index_of(z, y, x) * 4 + tp, to * 4 + tp))
    return out


def stay(x):
    return pltpu.with_memory_space_constraint(x, pltpu.HBM)


def call(kernel, out, ins, outs, args, scratch=(), mib=56, flops=10**7, nbytes=MIB):
    return pl.pallas_call(
        kernel,
        out_shape=out,
        in_specs=ins,
        out_specs=outs,
        scratch_shapes=scratch,
        compiler_params=params(mib),
        cost_estimate=pl.CostEstimate(flops=flops, bytes_accessed=nbytes, transcendentals=0),
    )(*args)


def layer(tokens, order, gain_attn, gain_ffn, w_query, w_key, w_value, w_out, w_gate, w_up, w_down):
    rows, width = tokens.shape
    me, tp = place()
    every = ("blk", "tp")
    order = stay(order)
    table = jnp.asarray(angles())
    trig = sds((rows, 128), F32)
    half = sds((2 * HALF, 128))
    dma = pltpu.SemaphoreType.DMA

    normed, mine, send, cos, sin = call(
        kv_kernel,
        [sds((rows, width)), half, half, trig, trig],
        [SM, ANY, ANY, ANY, ANY, ANY], [VM] * 5,
        (order, stay(tokens), stay(gain_attn[None, :]), stay(w_key), stay(w_value), stay(table)),
        [
            pltpu.VMEM((2, 2 * HALF, 128), BF),
            pltpu.VMEM(tokens.shape, BF),
            pltpu.VMEM((1, width), F32),
            pltpu.VMEM((width, 256), BF),
            pltpu.VMEM(table.shape, F32),
            dma((10,)),
        ],
        mib=14,
    )
    got = lax.ppermute(send, "tp", CORES)
    one = call(pack_kernel, sds((2, 2 * HALF, 128)), [VM] * 2, VM, (mine[None], got[None]), mib=4)
    other = lax.ppermute(one, "blk", FLIP_X)
    two = call(
        pack_kernel, sds((2, 2, 2 * HALF, 128)), [VM] * 2, VM, (one[None], other[None]), mib=4
    )
    near = [lax.ppermute(two, every, along(False, k)) for k in STEPS]
    eight = call(pack_kernel, sds((8, 2, 2 * HALF, 128)), [VM] * 4, VM, (two, *near), mib=8)
    q = call(
        q_kernel, sds((2, 128, 1024)),
        [VM, ANY, VM, VM], VM,
        (normed, w_query, cos, sin),
        [pltpu.VMEM(w_query.shape, BF), dma((4,))],
        mib=16, flops=10**9, nbytes=4 * MIB,
    )
    q2 = lax.ppermute(q, "tp", CORES)
    wo2 = lax.ppermute(w_out, "tp", CORES)
    wx = lax.ppermute(lax.optimization_barrier((w_out, two))[0], "tp", CHIPS)
    wx2 = lax.ppermute(wx, "tp", CORES)
    far = [lax.ppermute(eight, every, along(True, k)) for k in BACK[:2]]
    far.append(lax.ppermute(far[0], every, along(True, 3)))

    state = [sds((4, 1, 1024), F32), sds((4, 80, 1024), F32)]
    m, acc = call(
        start_kernel, state, [SM] + [VM] * 3, [VM] * 2, (order, q, q2, eight),
        mib=16, flops=2 * 10**9, nbytes=2 * MIB,
    )
    for j in range(2):
        m, acc = call(
            functools.partial(next_kernel, BACK[j]), state,
            [SM] + [VM] * 5, [VM] * 2, (order, q, q2, far[j], m, acc),
            mib=16, flops=2 * 10**9, nbytes=2 * MIB,
        )
    keep, send = call(
        functools.partial(last_kernel, BACK[2]), [sds((4, 80, 512), F32)] * 2,
        [SM] + [VM] * 5, [VM] * 2, (order, q, q2, far[2], m, acc),
        [pltpu.VMEM(s.shape, F32) for s in state],
        mib=16, flops=2 * 10**9, nbytes=2 * MIB,
    )
    got = lax.ppermute(send, "tp", CORES)
    heads = call(join_kernel, sds((HALF, 2 * w_out.shape[0])), [VM] * 2, VM, (keep, got), mib=8)
    there = lax.ppermute(heads, "tp", CHIPS)
    here = call(
        project_kernel, sds((HALF, width), F32), [VM] * 3, VM, (heads, w_out, wo2),
        mib=8, flops=10**9, nbytes=4 * MIB,
    )
    weights = (w_gate, w_up, w_down)
    weights = [pltpu.with_memory_space_constraint(w, pltpu.VMEM) for w in weights]
    share = width // lax.axis_size("tp")
    gain = gain_ffn[None, :]
    part = sds((HALF, width))
    slab = sds((rows, share))
    wide = sds((rows, share), F32)
    thin = sds((HALF, share), F32)
    att, normed, own = call(
        own_kernel, [part, part, thin], [VM] * 6, [VM] * 3,
        (here, there, wx, wx2, tokens, gain),
        [pltpu.VMEM((HALF, width), F32)], mib=8,
    )
    att = lax.ppermute(att, "tp", CORES)
    hidden = call(hidden_kernel, part, [VM] * 3, VM, (normed, *weights[:2]), mib=8, flops=2 * 10**9)
    other, hidden, keep, send = call(
        away_kernel, [thin, sds((rows, width)), wide, slab], [VM] * 7, [VM] * 4,
        (tokens, att, gain, hidden, *weights),
        [pltpu.VMEM((HALF, width), BF), pltpu.VMEM((HALF, width), F32)],
        mib=14, flops=4 * 10**9,
    )
    got = lax.ppermute(send, "tp", CORES)
    away = call(sum_kernel, slab, [VM] * 2, VM, (keep, got), mib=4)
    far_sum = lax.ppermute(away, "tp", CHIPS)
    keep, send = call(
        home_kernel, [wide, slab], [VM] * 4, [VM] * 2, (hidden, weights[2], own, other),
        mib=10, flops=10**9,
    )
    near_sum = lax.ppermute(send, "tp", CORES)
    return call(final_kernel, slab, [VM] * 3, VM, (keep, near_sum, far_sum), mib=8)


def solution(mesh):
    placed = (
        P("blk", None),
        P(),
        P(),
        P(),
        P(None, "tp"),
        P(None, "tp"),
        P(None, "tp"),
        P("tp", None),
        P(None, "tp"),
        P(None, "tp"),
        P("tp", None),
    )
    return jax.shard_map(
        layer, mesh=mesh, in_specs=placed, out_specs=P("blk", "tp"), check_vma=False
    )
```

```python
import functools
import math

import jax
import jax.numpy as jnp
import numpy as np
from jax import lax
from jax.experimental import pallas as pl
from jax.experimental.pallas import tpu as pltpu
from jax.sharding import PartitionSpec as P


HD = 64
EPS = 1e-05
ROPE_BASE = 500000.0
COLUMNS = (0, 1, 3)
NEG = -1e30
HIDDEN = -2e30
HALF = 128
LOG2E = math.log2(math.e)
MIB = 2**20

VM = pl.BlockSpec(memory_space=pltpu.VMEM)
SM = pl.BlockSpec(memory_space=pltpu.SMEM)
ANY = pl.BlockSpec(memory_space=pltpu.HBM)
BF = jnp.bfloat16
F32 = jnp.float32


def params(mib):
    return pltpu.CompilerParams(vmem_limit_bytes=mib * MIB)


def dot(a, b):
    return jnp.dot(a, b, preferred_element_type=F32)


def rope(u, cos, sin):
    n = u.shape[1] // 128
    outs = []
    lane = lax.broadcasted_iota(jnp.int32, (u.shape[0], 128), 1)
    low = lane % HD < HD // 2
    for k in range(n):
        v = u[:, k * 128 : (k + 1) * 128]
        other = jnp.where(low, pltpu.roll(v, 128 - HD // 2, 1), pltpu.roll(v, HD // 2, 1))
        outs.append(v * cos + other * sin)
    return outs


def angles():
    freq = ROPE_BASE ** (-(np.arange(HD // 2, dtype=np.float64) * 2.0 / HD))
    freq = np.tile(freq, 4)[None, :]
    near = np.arange(HALF, dtype=np.float64)[:, None] * freq
    far = np.arange(64, dtype=np.float64)[:, None] * HALF * freq
    return np.concatenate([np.cos(near), np.sin(near), np.cos(far), np.sin(far)]).astype(np.float32)


def place():
    me = lax.axis_index("blk").astype(jnp.int32)
    tp = lax.axis_index("tp").astype(jnp.int32)
    return me, tp


def kv_kernel(
    order_ref, tok_hbm, gain_hbm, wk_hbm, wv_hbm, table_hbm,
    normed_ref, mine_ref, send_ref, cos_ref, sin_ref,
    kv_ref, tok_ref, gain_ref, w_ref, table_ref, sems,
):
    rows = 64
    n = tok_ref.shape[0] // rows
    gain_copy = pltpu.make_async_copy(gain_hbm, gain_ref, sems.at[9])
    gain_copy.start()
    copies = []
    for i in range(n):
        part = slice(i * rows, (i + 1) * rows)
        copies.append(pltpu.make_async_copy(tok_hbm.at[part], tok_ref.at[part], sems.at[i]))
    half = w_ref.shape[0] // 2
    for i, a in enumerate((wk_hbm, wv_hbm)):
        b = w_ref.at[:, i * 128 : (i + 1) * 128]
        for part in (slice(0, half), slice(half, 2 * half)):
            copies.append(pltpu.make_async_copy(a.at[part], b.at[part], sems.at[len(copies)]))
    copies.append(pltpu.make_async_copy(table_hbm, table_ref, sems.at[len(copies)]))
    for c in copies:
        c.start()
    me, tp = place()
    core = tp % 2
    gain_copy.wait()
    for r in range(0, n * rows, rows):
        copies[r // rows].wait()
        x = tok_ref[r : r + rows, :].astype(F32)
        scale = lax.rsqrt(jnp.mean(x * x, axis=-1, keepdims=True) + EPS)
        normed_ref[r : r + rows, :] = (x * scale * gain_ref[...]).astype(BF)
    copies[-1].wait()
    lane = lax.broadcasted_iota(jnp.int32, (HALF, 128), 1)
    sign = jnp.where(lane % HD < HD // 2, -1.0, 1.0).astype(F32)
    cos, sin = table_ref[:HALF, :], table_ref[HALF : 2 * HALF, :]
    for j in range(2):
        b = order_ref[2 * me + j]
        cb, sb = table_ref[pl.ds(256 + b, 1), :], table_ref[pl.ds(320 + b, 1), :]
        cos_ref[j * HALF : (j + 1) * HALF, :] = cos * cb - sin * sb
        sin_ref[j * HALF : (j + 1) * HALF, :] = (sin * cb + cos * sb) * sign
    for i in range(4):
        copies[n + i].wait()
    both = dot(normed_ref[...], w_ref[...])
    k = rope(both[:, :128], cos_ref[...], sin_ref[...])[0].astype(BF)
    v = jnp.transpose(both[:, 128:]).astype(BF)
    for j in range(2):
        kv_ref[j, :HALF, :] = k[j * HALF : (j + 1) * HALF]
        kv_ref[j, HALF:, :] = v[:, j * HALF : (j + 1) * HALF]
    mine_ref[...] = kv_ref[core]
    send_ref[...] = kv_ref[1 - core]


def pack_kernel(*refs):
    out = refs[-1]
    at = 0
    for r in refs[:-1]:
        out[at : at + r.shape[0]] = r[...]
        at += r.shape[0]


def q_kernel(normed_ref, wq_hbm, cos_ref, sin_ref, q_ref, wq_ref, sem):
    part = wq_ref.shape[0] // 4
    copies = []
    for i in range(4):
        at = slice(i * part, (i + 1) * part)
        copies.append(pltpu.make_async_copy(wq_hbm.at[at], wq_ref.at[at], sem.at[i]))
    for c in copies:
        c.start()
    for c in copies:
        c.wait()
    q = dot(normed_ref[...], wq_ref[...])
    parts = rope(q, cos_ref[...], sin_ref[...])
    q_ref[...] = jnp.zeros(q_ref.shape, BF)
    for k, part in enumerate(parts):
        t = jnp.transpose(part * (HD**-0.5 * LOG2E)).astype(BF)
        for a in range(2):
            head = 2 * k + a
            h, g = head // 4, head % 4
            for i in range(2):
                q_ref[h, h * HD : (h + 1) * HD, i * 512 + g * 128 : i * 512 + (g + 1) * 128] = t[
                    a * HD : (a + 1) * HD, i * HALF : (i + 1) * HALF
                ]


def attend(order_ref, blocks, own, q_refs, m_in, acc_in, m_ref, acc_ref):
    me, tp = place()
    core = tp % 2
    width = 256
    pq = [order_ref[2 * me + i] for i in range(2)]
    z, y, x = me // 8, me // 2 % 4, me % 2
    pos = []
    for _, _, d, k, flip in blocks:
        zz = (z + 4 - jnp.where(core == 0, d, k)) % 4
        yy = (y + 4 - jnp.where(core == 0, k, d)) % 4
        xx = 1 - x if flip else x
        pos.append(order_ref[2 * (zz * 8 + yy * 2 + xx) + core])
    adds = [[jnp.where(p < q, jnp.float32(0.0), jnp.float32(HIDDEN)) for p in pos] for q in pq]
    if own:
        key = lax.broadcasted_iota(jnp.int32, (HALF, width), 0)
        tok = lax.broadcasted_iota(jnp.int32, (HALF, width), 1) % HALF
        tri = jnp.where(key <= tok, 0.0, HIDDEN).astype(F32)

    def scores(p, h, t):
        keys = jnp.concatenate([r[g, p, :HALF, :] for r, g, _, _, _ in blocks], axis=0)
        return dot(keys, q_refs[p][h, :, t * width : (t + 1) * width])

    def rest(p, h, t, s):
        sl = slice(t * width, (t + 1) * width)
        i = t * width // 512
        add = adds[i]
        parts = [s[g * HALF : (g + 1) * HALF] for g in range(len(blocks))]
        if own:
            parts[0] = parts[0] + jnp.where(core == i, tri, add[0])
            add = [jnp.float32(0.0), *add[1:]]
        m_old = jnp.full((1, width), NEG, F32) if own else m_in[2 * p + h, :, sl]
        m_new = m_old
        for v, b in zip(parts, add):
            m_new = jnp.maximum(m_new, jnp.max(v, axis=0, keepdims=True) + b)
        e = [jnp.exp2(v + (b - m_new)).astype(BF) for v, b in zip(parts, add)]
        vt = [r[g, p, HALF + h * HD : HALF + (h + 1) * HD, :] for r, g, _, _, _ in blocks]
        vt = jnp.concatenate(vt, axis=1)
        vt = jnp.concatenate([vt, jnp.ones((16, vt.shape[1]), BF)], axis=0)
        new = dot(vt, jnp.concatenate(e, axis=0))
        if not own:
            new = acc_in[2 * p + h, :, sl] * jnp.exp2(m_old - m_new) + new
        acc_ref[2 * p + h, :, sl] = new
        m_ref[2 * p + h, :, sl] = m_new

    waiting = []
    for p in range(2):
        for h in range(2):
            for t in range(1024 // width):
                waiting.append((p, h, t, scores(p, h, t)))
                if len(waiting) > 3:
                    rest(*waiting.pop(0))
    for w in waiting:
        rest(*w)


def all_of(ref, columns, k):
    return [(ref, 2 * i + f, d, k, f == 1) for i, d in enumerate(columns) for f in range(2)]


def start_kernel(order_ref, q_ref, q2_ref, kv_ref, m_ref, acc_ref):
    blocks = all_of(kv_ref, COLUMNS, 0)
    attend(order_ref, blocks, True, (q_ref, q2_ref), None, None, m_ref, acc_ref)


def next_kernel(places, order_ref, q_ref, q2_ref, *refs):
    n = len(places)
    m_in, acc_in, m_ref, acc_ref = refs[n:]
    blocks = [b for r, (d, k) in zip(refs, places) for b in all_of(r, d, k)]
    attend(order_ref, blocks, False, (q_ref, q2_ref), m_in, acc_in, m_ref, acc_ref)


def last_kernel(places, order_ref, q_ref, q2_ref, *refs):
    n = len(places)
    m_in, acc_in, keep_ref, send_ref, m_ref, acc_ref = refs[n:]
    next_kernel(places, order_ref, q_ref, q2_ref, *refs[:n], m_in, acc_in, m_ref, acc_ref)
    core = place()[1] % 2
    for ref, i in ((keep_ref, core), (send_ref, 1 - core)):
        at = pl.ds(pl.multiple_of(i * 512, 512), 512)
        for j in range(4):
            ref[j, :72, :] = acc_ref[j, :72, at]
            ref[j, 72:, :] = jnp.broadcast_to(m_ref[j, :, at], (8, 512))


def join_kernel(mine_ref, got_ref, heads_ref):
    for p in range(2):
        for h in range(2):
            a, b = 2 * p + h, 2 * (1 - p) + h
            ma, mb = mine_ref[a, 72:73, :], got_ref[b, 72:73, :]
            m = jnp.maximum(ma, mb)
            fa, fb = jnp.exp2(ma - m), jnp.exp2(mb - m)
            low = mine_ref[a, HD : HD + 1, :] * fa + got_ref[b, HD : HD + 1, :] * fb
            value = (mine_ref[a, :HD, :] * fa + got_ref[b, :HD, :] * fb) / low
            for k in range(2):
                both = jnp.concatenate(
                    [value[:, (2 * k + g) * 128 : (2 * k + g + 1) * 128] for g in range(2)], axis=0
                )
                col = (p * 4 + h * 2 + k) * 128
                heads_ref[:, col : col + 128] = jnp.transpose(both).astype(BF)


def project_kernel(heads_ref, wo_ref, wo2_ref, out_ref):
    half = wo_ref.shape[0]
    out_ref[...] = dot(heads_ref[:, :half], wo_ref[...]) + dot(heads_ref[:, half:], wo2_ref[...])


def rows_of(i):
    return pl.ds(pl.multiple_of(i * HALF, HALF), HALF)


def normalize(x, gain_ref):
    scale = lax.rsqrt(jnp.mean(x * x, axis=-1, keepdims=True) + EPS)
    return (x * scale * gain_ref[...]).astype(BF)


def residual_rows(tok_ref, att_ref, gain_ref, block, normed_ref, resid_ref, full_ref):
    rows = 64
    start = pl.multiple_of(block * HALF, HALF)
    for r in range(0, HALF, rows):
        x = tok_ref[pl.ds(start + r, rows), :].astype(F32) + att_ref[r : r + rows, :].astype(F32)
        full_ref[r : r + rows, :] = x
        normed_ref[r : r + rows, :] = normalize(x, gain_ref)
    share = resid_ref.shape[1]
    tp = place()[1]
    resid_ref[...] = full_ref[:, pl.ds(pl.multiple_of(tp * share, share), share)]


def own_kernel(
    part_ref, heads_ref, wo_ref, wo2_ref, tok_ref, gain_ref, att_ref, normed_ref, resid_ref, full_ref
):
    half = wo_ref.shape[0]
    att = part_ref[...] + dot(heads_ref[:, :half], wo_ref[...])
    att_ref[...] = (att + dot(heads_ref[:, half:], wo2_ref[...])).astype(BF)
    core = place()[1] % 2
    residual_rows(tok_ref, att_ref, gain_ref, core, normed_ref, resid_ref, full_ref)


def gated(normed, wg, wu, store):
    tf = 512

    def body(t, carry):
        c = pl.ds(pl.multiple_of(t * tf, tf), tf)
        gate = dot(normed[...], wg[:, c])
        up = dot(normed[...], wu[:, c])
        store(c, (gate / (1.0 + jnp.exp(-gate)) * up).astype(BF))
        return carry

    lax.fori_loop(0, wg.shape[1] // tf, body, 0)


def hidden_kernel(normed_ref, wg, wu, hidden_ref):
    def store(c, value):
        hidden_ref[:, c] = value

    gated(normed_ref, wg, wu, store)


def down_slice(hidden_ref, wd, i):
    return dot(hidden_ref[...], wd[:, pl.ds(pl.multiple_of(i * 512, 512), 512)])


def away_kernel(
    tok_ref, att_ref, gain_ref, mine_ref, wg, wu, wd,
    resid_ref, hidden_ref, keep_ref, send_ref,
    normed_ref, full_ref,
):
    tp = place()[1]
    core, chip = tp % 2, tp // 2
    residual_rows(tok_ref, att_ref, gain_ref, 1 - core, normed_ref, resid_ref, full_ref)
    hidden_ref[rows_of(core), :] = mine_ref[...]

    def store(c, value):
        hidden_ref[rows_of(1 - core), c] = value

    gated(normed_ref, wg, wu, store)
    keep_ref[...] = down_slice(hidden_ref, wd, 2 * (1 - chip) + core)
    send_ref[...] = down_slice(hidden_ref, wd, 2 * (1 - chip) + 1 - core).astype(BF)


def home_kernel(hidden_ref, wd, own_ref, other_ref, keep_ref, send_ref):
    tp = place()[1]
    core, chip = tp % 2, tp // 2
    part = down_slice(hidden_ref, wd, 2 * chip + core)
    keep_ref[...] = part
    for i, ref in ((core, own_ref), (1 - core, other_ref)):
        keep_ref[rows_of(i), :] += ref[...]
    send_ref[...] = down_slice(hidden_ref, wd, 2 * chip + 1 - core).astype(BF)


def final_kernel(keep_ref, a_ref, b_ref, out_ref):
    out_ref[...] = (keep_ref[...] + a_ref[...].astype(F32) + b_ref[...].astype(F32)).astype(BF)


def sum_kernel(a_ref, b_ref, out_ref):
    out_ref[...] = (a_ref[...].astype(F32) + b_ref[...].astype(F32)).astype(BF)


def sds(shape, dtype=BF):
    return jax.ShapeDtypeStruct(shape, dtype)


def index_of(z, y, x):
    return z % 4 * 8 + y % 4 * 2 + x


GRID = [(z, y, x) for z in range(4) for y in range(4) for x in range(2)]
FLIP_X = [(index_of(z, y, x), index_of(z, y, 1 - x)) for z, y, x in GRID]
CORES = [(0, 1), (1, 0), (2, 3), (3, 2)]
CHIPS = [(0, 2), (2, 0), (1, 3), (3, 1)]


def along(second, k):
    out = []
    for z, y, x in GRID:
        for tp in range(4):
            if (tp % 2 == 0) != second:
                to = index_of(z + k, y, x)
            else:
                to = index_of(z, y + k, x)
            out.append((index_of(z, y, x) * 4 + tp, to * 4 + tp))
    return out


def stay(x):
    return pltpu.with_memory_space_constraint(x, pltpu.HBM)


def call(kernel, out, ins, outs, args, scratch=(), mib=56, flops=10**7, nbytes=MIB):
    return pl.pallas_call(
        kernel,
        out_shape=out,
        in_specs=ins,
        out_specs=outs,
        scratch_shapes=scratch,
        compiler_params=params(mib),
        cost_estimate=pl.CostEstimate(flops=flops, bytes_accessed=nbytes, transcendentals=0),
    )(*args)


def layer(tokens, order, gain_attn, gain_ffn, w_query, w_key, w_value, w_out, w_gate, w_up, w_down):
    rows, width = tokens.shape
    me, tp = place()
    every = ("blk", "tp")
    order = stay(order)
    table = jnp.asarray(angles())
    trig = sds((rows, 128), F32)
    half = sds((2 * HALF, 128))
    dma = pltpu.SemaphoreType.DMA

    normed, mine, send, cos, sin = call(
        kv_kernel,
        [sds((rows, width)), half, half, trig, trig],
        [SM, ANY, ANY, ANY, ANY, ANY], [VM] * 5,
        (order, stay(tokens), stay(gain_attn[None, :]), stay(w_key), stay(w_value), stay(table)),
        [
            pltpu.VMEM((2, 2 * HALF, 128), BF),
            pltpu.VMEM(tokens.shape, BF),
            pltpu.VMEM((1, width), F32),
            pltpu.VMEM((width, 256), BF),
            pltpu.VMEM(table.shape, F32),
            dma((10,)),
        ],
        mib=14,
    )
    got = lax.ppermute(send, "tp", CORES)
    one = call(pack_kernel, sds((2, 2 * HALF, 128)), [VM] * 2, VM, (mine[None], got[None]), mib=4)
    other = lax.ppermute(one, "blk", FLIP_X)
    two = call(
        pack_kernel, sds((2, 2, 2 * HALF, 128)), [VM] * 2, VM, (one[None], other[None]), mib=4
    )
    near = [lax.ppermute(two, every, along(False, k)) for k in COLUMNS[1:]]
    six = call(pack_kernel, sds((6, 2, 2 * HALF, 128)), [VM] * 3, VM, (two, *near), mib=8)
    column = lax.ppermute(near[1], every, along(False, 3))
    q = call(
        q_kernel, sds((2, 128, 1024)),
        [VM, ANY, VM, VM], VM,
        (normed, w_query, cos, sin),
        [pltpu.VMEM(w_query.shape, BF), dma((4,))],
        mib=16, flops=10**9, nbytes=4 * MIB,
    )
    q2 = lax.ppermute(q, "tp", CORES)
    wo2 = lax.ppermute(w_out, "tp", CORES)
    wx = lax.ppermute(w_out, "tp", CHIPS)
    wx2 = lax.ppermute(wx, "tp", CORES)
    far = {k: lax.ppermute(six, every, along(True, k)) for k in (3, 1)}
    side = {k: lax.ppermute(column, every, along(True, k)) for k in (3, 1)}
    far[2] = lax.ppermute(far[3], every, along(True, 3))
    side[2] = lax.ppermute(side[3], every, along(True, 3))
    side[0] = column

    state = [sds((4, 1, 1024), F32), sds((4, 80, 1024), F32)]
    m, acc = call(
        start_kernel, state, [SM] + [VM] * 3, [VM] * 2, (order, q, q2, six),
        mib=14, flops=2 * 10**9, nbytes=2 * MIB,
    )

    def add(kernel, parts, out, scratch=()):
        places = [((2,) if s is side else COLUMNS, k) for s, k in parts]
        return call(
            functools.partial(kernel, places), out,
            [SM] + [VM] * (4 + len(parts)), [VM] * 2,
            (order, q, q2, *[s[k] for s, k in parts], m, acc), scratch,
            mib=14, flops=2 * 10**9, nbytes=2 * MIB,
        )

    m, acc = add(next_kernel, [(far, 3)], state)
    m, acc = add(next_kernel, [(far, 1)], state)
    m, acc = add(next_kernel, [(side, 0), (side, 3), (side, 1)], state)
    keep, send = add(
        last_kernel, [(far, 2), (side, 2)], [sds((4, 80, 512), F32)] * 2,
        [pltpu.VMEM(s.shape, F32) for s in state],
    )
    got = lax.ppermute(send, "tp", CORES)
    heads = call(join_kernel, sds((HALF, 2 * w_out.shape[0])), [VM] * 2, VM, (keep, got), mib=8)
    there = lax.ppermute(heads, "tp", CHIPS)
    here = call(
        project_kernel, sds((HALF, width), F32), [VM] * 3, VM, (heads, w_out, wo2),
        mib=8, flops=10**9, nbytes=4 * MIB,
    )
    weights = (w_gate, w_up, w_down)
    weights = [pltpu.with_memory_space_constraint(w, pltpu.VMEM) for w in weights]
    share = width // lax.axis_size("tp")
    gain = gain_ffn[None, :]
    part = sds((HALF, width))
    slab = sds((rows, share))
    wide = sds((rows, share), F32)
    thin = sds((HALF, share), F32)
    att, normed, own = call(
        own_kernel, [part, part, thin], [VM] * 6, [VM] * 3,
        (here, there, wx, wx2, tokens, gain),
        [pltpu.VMEM((HALF, width), F32)], mib=8,
    )
    att = lax.ppermute(att, "tp", CORES)
    hidden = call(hidden_kernel, part, [VM] * 3, VM, (normed, *weights[:2]), mib=8, flops=2 * 10**9)
    other, hidden, keep, send = call(
        away_kernel, [thin, sds((rows, width)), wide, slab], [VM] * 7, [VM] * 4,
        (tokens, att, gain, hidden, *weights),
        [pltpu.VMEM((HALF, width), BF), pltpu.VMEM((HALF, width), F32)],
        mib=14, flops=4 * 10**9,
    )
    got = lax.ppermute(send, "tp", CORES)
    away = call(sum_kernel, slab, [VM] * 2, VM, (keep, got), mib=4)
    far_sum = lax.ppermute(away, "tp", CHIPS)
    keep, send = call(
        home_kernel, [wide, slab], [VM] * 4, [VM] * 2, (hidden, weights[2], own, other),
        mib=10, flops=10**9,
    )
    near_sum = lax.ppermute(send, "tp", CORES)
    return call(final_kernel, slab, [VM] * 3, VM, (keep, near_sum, far_sum), mib=8)


def solution(mesh):
    placed = (
        P("blk", None),
        P(),
        P(),
        P(),
        P(None, "tp"),
        P(None, "tp"),
        P(None, "tp"),
        P("tp", None),
        P(None, "tp"),
        P(None, "tp"),
        P("tp", None),
    )
    return jax.shard_map(
        layer, mesh=mesh, in_specs=placed, out_specs=P("blk", "tp"), check_vma=False
    )
```

```python
import functools
import math

import jax
import jax.numpy as jnp
import numpy as np
from jax import lax
from jax.experimental import pallas as pl
from jax.experimental.pallas import tpu as pltpu
from jax.sharding import PartitionSpec as P


HD = 64
EPS = 1e-05
ROPE_BASE = 500000.0
COLUMNS = (0, 1, 3)
NEG = -1e30
HIDDEN = -2e30
HALF = 128
LOG2E = math.log2(math.e)
MIB = 2**20

VM = pl.BlockSpec(memory_space=pltpu.VMEM)
SM = pl.BlockSpec(memory_space=pltpu.SMEM)
ANY = pl.BlockSpec(memory_space=pltpu.HBM)
BF = jnp.bfloat16
F32 = jnp.float32


def params(mib):
    return pltpu.CompilerParams(vmem_limit_bytes=mib * MIB)


def dot(a, b):
    return jnp.dot(a, b, preferred_element_type=F32)


def rope(u, cos, sin):
    n = u.shape[1] // 128
    outs = []
    lane = lax.broadcasted_iota(jnp.int32, (u.shape[0], 128), 1)
    low = lane % HD < HD // 2
    for k in range(n):
        v = u[:, k * 128 : (k + 1) * 128]
        other = jnp.where(low, pltpu.roll(v, 128 - HD // 2, 1), pltpu.roll(v, HD // 2, 1))
        outs.append(v * cos + other * sin)
    return outs


def angles():
    freq = ROPE_BASE ** (-(np.arange(HD // 2, dtype=np.float64) * 2.0 / HD))
    freq = np.tile(freq, 4)[None, :]
    near = np.arange(HALF, dtype=np.float64)[:, None] * freq
    far = np.arange(64, dtype=np.float64)[:, None] * HALF * freq
    return np.concatenate([np.cos(near), np.sin(near), np.cos(far), np.sin(far)]).astype(np.float32)


def place():
    me = lax.axis_index("blk").astype(jnp.int32)
    tp = lax.axis_index("tp").astype(jnp.int32)
    return me, tp


def kv_kernel(
    order_ref, tok_hbm, gain_hbm, wk_hbm, wv_hbm, table_hbm,
    normed_ref, mine_ref, send_ref, cos_ref, sin_ref,
    kv_ref, tok_ref, gain_ref, w_ref, table_ref, sems,
):
    rows = 64
    n = tok_ref.shape[0] // rows
    gain_copy = pltpu.make_async_copy(gain_hbm, gain_ref, sems.at[9])
    gain_copy.start()
    copies = []
    for i in range(n):
        part = slice(i * rows, (i + 1) * rows)
        copies.append(pltpu.make_async_copy(tok_hbm.at[part], tok_ref.at[part], sems.at[i]))
    half = w_ref.shape[0] // 2
    for i, a in enumerate((wk_hbm, wv_hbm)):
        b = w_ref.at[:, i * 128 : (i + 1) * 128]
        for part in (slice(0, half), slice(half, 2 * half)):
            copies.append(pltpu.make_async_copy(a.at[part], b.at[part], sems.at[len(copies)]))
    copies.append(pltpu.make_async_copy(table_hbm, table_ref, sems.at[len(copies)]))
    for c in copies:
        c.start()
    me, tp = place()
    core = tp % 2
    gain_copy.wait()
    for r in range(0, n * rows, rows):
        copies[r // rows].wait()
        x = tok_ref[r : r + rows, :].astype(F32)
        scale = lax.rsqrt(jnp.mean(x * x, axis=-1, keepdims=True) + EPS)
        normed_ref[r : r + rows, :] = (x * scale * gain_ref[...]).astype(BF)
    copies[-1].wait()
    lane = lax.broadcasted_iota(jnp.int32, (HALF, 128), 1)
    sign = jnp.where(lane % HD < HD // 2, -1.0, 1.0).astype(F32)
    cos, sin = table_ref[:HALF, :], table_ref[HALF : 2 * HALF, :]
    for j in range(2):
        b = order_ref[2 * me + j]
        cb, sb = table_ref[pl.ds(256 + b, 1), :], table_ref[pl.ds(320 + b, 1), :]
        cos_ref[j * HALF : (j + 1) * HALF, :] = cos * cb - sin * sb
        sin_ref[j * HALF : (j + 1) * HALF, :] = (sin * cb + cos * sb) * sign
    for i in range(4):
        copies[n + i].wait()
    both = dot(normed_ref[...], w_ref[...])
    k = rope(both[:, :128], cos_ref[...], sin_ref[...])[0].astype(BF)
    v = jnp.transpose(both[:, 128:]).astype(BF)
    for j in range(2):
        kv_ref[j, :HALF, :] = k[j * HALF : (j + 1) * HALF]
        kv_ref[j, HALF:, :] = v[:, j * HALF : (j + 1) * HALF]
    mine_ref[...] = kv_ref[core]
    send_ref[...] = kv_ref[1 - core]


def pack_kernel(*refs):
    out = refs[-1]
    at = 0
    for r in refs[:-1]:
        out[at : at + r.shape[0]] = r[...]
        at += r.shape[0]


def q_kernel(normed_ref, wq_hbm, cos_ref, sin_ref, q_ref, wq_ref, sem):
    part = wq_ref.shape[0] // 4
    copies = []
    for i in range(4):
        at = slice(i * part, (i + 1) * part)
        copies.append(pltpu.make_async_copy(wq_hbm.at[at], wq_ref.at[at], sem.at[i]))
    for c in copies:
        c.start()
    for c in copies:
        c.wait()
    q = dot(normed_ref[...], wq_ref[...])
    parts = rope(q, cos_ref[...], sin_ref[...])
    q_ref[...] = jnp.zeros(q_ref.shape, BF)
    for k, part in enumerate(parts):
        t = jnp.transpose(part * (HD**-0.5 * LOG2E)).astype(BF)
        for a in range(2):
            head = 2 * k + a
            h, g = head // 4, head % 4
            for i in range(2):
                q_ref[h, h * HD : (h + 1) * HD, i * 512 + g * 128 : i * 512 + (g + 1) * 128] = t[
                    a * HD : (a + 1) * HD, i * HALF : (i + 1) * HALF
                ]


def attend(order_ref, blocks, own, q_refs, m_in, acc_in, m_ref, acc_ref):
    me, tp = place()
    core = tp % 2
    width = 256
    pq = [order_ref[2 * me + i] for i in range(2)]
    z, y, x = me // 8, me // 2 % 4, me % 2
    pos = []
    for _, _, d, k, flip in blocks:
        zz = (z + 4 - jnp.where(core == 0, d, k)) % 4
        yy = (y + 4 - jnp.where(core == 0, k, d)) % 4
        xx = 1 - x if flip else x
        pos.append(order_ref[2 * (zz * 8 + yy * 2 + xx) + core])
    adds = [[jnp.where(p < q, jnp.float32(0.0), jnp.float32(HIDDEN)) for p in pos] for q in pq]
    if own:
        key = lax.broadcasted_iota(jnp.int32, (HALF, width), 0)
        tok = lax.broadcasted_iota(jnp.int32, (HALF, width), 1) % HALF
        tri = jnp.where(key <= tok, 0.0, HIDDEN).astype(F32)

    def scores(p, h, t):
        keys = jnp.concatenate([r[g, p, :HALF, :] for r, g, _, _, _ in blocks], axis=0)
        return dot(keys, q_refs[p][h, :, t * width : (t + 1) * width])

    def rest(p, h, t, s):
        sl = slice(t * width, (t + 1) * width)
        i = t * width // 512
        add = adds[i]
        parts = [s[g * HALF : (g + 1) * HALF] for g in range(len(blocks))]
        if own:
            parts[0] = parts[0] + jnp.where(core == i, tri, add[0])
            add = [jnp.float32(0.0), *add[1:]]
        m_old = jnp.full((1, width), NEG, F32) if own else m_in[2 * p + h, :, sl]
        m_new = m_old
        for v, b in zip(parts, add):
            m_new = jnp.maximum(m_new, jnp.max(v, axis=0, keepdims=True) + b)
        e = [jnp.exp2(v + (b - m_new)).astype(BF) for v, b in zip(parts, add)]
        vt = [r[g, p, HALF + h * HD : HALF + (h + 1) * HD, :] for r, g, _, _, _ in blocks]
        vt = jnp.concatenate(vt, axis=1)
        vt = jnp.concatenate([vt, jnp.ones((16, vt.shape[1]), BF)], axis=0)
        new = dot(vt, jnp.concatenate(e, axis=0))
        if not own:
            new = acc_in[2 * p + h, :, sl] * jnp.exp2(m_old - m_new) + new
        acc_ref[2 * p + h, :, sl] = new
        m_ref[2 * p + h, :, sl] = m_new

    waiting = []
    for p in range(2):
        for h in range(2):
            for t in range(1024 // width):
                waiting.append((p, h, t, scores(p, h, t)))
                if len(waiting) > 3:
                    rest(*waiting.pop(0))
    for w in waiting:
        rest(*w)


def all_of(ref, columns, k):
    return [(ref, 2 * i + f, d, k, f == 1) for i, d in enumerate(columns) for f in range(2)]


def start_kernel(order_ref, q_ref, q2_ref, kv_ref, m_ref, acc_ref):
    blocks = all_of(kv_ref, COLUMNS, 0)
    attend(order_ref, blocks, True, (q_ref, q2_ref), None, None, m_ref, acc_ref)


def next_kernel(places, order_ref, q_ref, q2_ref, *refs):
    n = len(places)
    m_in, acc_in, m_ref, acc_ref = refs[n:]
    blocks = [b for r, (d, k) in zip(refs, places) for b in all_of(r, d, k)]
    attend(order_ref, blocks, False, (q_ref, q2_ref), m_in, acc_in, m_ref, acc_ref)


def last_kernel(places, order_ref, q_ref, q2_ref, *refs):
    n = len(places)
    m_in, acc_in, keep_ref, send_ref, m_ref, acc_ref = refs[n:]
    next_kernel(places, order_ref, q_ref, q2_ref, *refs[:n], m_in, acc_in, m_ref, acc_ref)
    core = place()[1] % 2
    for ref, i in ((keep_ref, core), (send_ref, 1 - core)):
        at = pl.ds(pl.multiple_of(i * 512, 512), 512)
        for j in range(4):
            ref[j, :72, :] = acc_ref[j, :72, at]
            ref[j, 72:, :] = jnp.broadcast_to(m_ref[j, :, at], (8, 512))


def join_kernel(mine_ref, got_ref, heads_ref):
    for p in range(2):
        for h in range(2):
            a, b = 2 * p + h, 2 * (1 - p) + h
            ma, mb = mine_ref[a, 72:73, :], got_ref[b, 72:73, :]
            m = jnp.maximum(ma, mb)
            fa, fb = jnp.exp2(ma - m), jnp.exp2(mb - m)
            low = mine_ref[a, HD : HD + 1, :] * fa + got_ref[b, HD : HD + 1, :] * fb
            value = (mine_ref[a, :HD, :] * fa + got_ref[b, :HD, :] * fb) / low
            for k in range(2):
                both = jnp.concatenate(
                    [value[:, (2 * k + g) * 128 : (2 * k + g + 1) * 128] for g in range(2)], axis=0
                )
                col = (p * 4 + h * 2 + k) * 128
                heads_ref[:, col : col + 128] = jnp.transpose(both).astype(BF)


def project_kernel(heads_ref, wo_ref, wo2_ref, out_ref):
    half = wo_ref.shape[0]
    out_ref[...] = dot(heads_ref[:, :half], wo_ref[...]) + dot(heads_ref[:, half:], wo2_ref[...])


def rows_of(i):
    return pl.ds(pl.multiple_of(i * HALF, HALF), HALF)


def normalize(x, gain_ref):
    scale = lax.rsqrt(jnp.mean(x * x, axis=-1, keepdims=True) + EPS)
    return (x * scale * gain_ref[...]).astype(BF)


def residual_rows(tok_ref, att_ref, gain_ref, block, normed_ref, resid_ref, full_ref):
    rows = 64
    start = pl.multiple_of(block * HALF, HALF)
    for r in range(0, HALF, rows):
        x = tok_ref[pl.ds(start + r, rows), :].astype(F32) + att_ref[r : r + rows, :].astype(F32)
        full_ref[r : r + rows, :] = x
        normed_ref[r : r + rows, :] = normalize(x, gain_ref)
    share = resid_ref.shape[1]
    tp = place()[1]
    resid_ref[...] = full_ref[:, pl.ds(pl.multiple_of(tp * share, share), share)]


def own_kernel(
    part_ref, heads_ref, wo_ref, wo2_ref, tok_ref, gain_ref, att_ref, normed_ref, resid_ref, full_ref
):
    half = wo_ref.shape[0]
    att = part_ref[...] + dot(heads_ref[:, :half], wo_ref[...])
    att_ref[...] = (att + dot(heads_ref[:, half:], wo2_ref[...])).astype(BF)
    core = place()[1] % 2
    residual_rows(tok_ref, att_ref, gain_ref, core, normed_ref, resid_ref, full_ref)


def gated(normed, wg, wu, store):
    tf = 512
    waiting = []
    for t in range(wg.shape[1] // tf):
        c = slice(t * tf, (t + 1) * tf)
        waiting.append((c, dot(normed[...], wg[:, c]), dot(normed[...], wu[:, c])))
        if t > 0:
            activate(store, *waiting.pop(0))
    activate(store, *waiting.pop(0))


def activate(store, c, gate, up):
    store(c, (gate / (1.0 + jnp.exp(-gate)) * up).astype(BF))


def hidden_kernel(normed_ref, wg, wu, hidden_ref):
    def store(c, value):
        hidden_ref[:, c] = value

    gated(normed_ref, wg, wu, store)


def down_slice(hidden_ref, wd, i):
    return dot(hidden_ref[...], wd[:, pl.ds(pl.multiple_of(i * 512, 512), 512)])


def away_kernel(
    tok_ref, att_ref, gain_ref, mine_ref, wg, wu, wd,
    resid_ref, hidden_ref, keep_ref, send_ref,
    normed_ref, full_ref,
):
    tp = place()[1]
    core, chip = tp % 2, tp // 2
    residual_rows(tok_ref, att_ref, gain_ref, 1 - core, normed_ref, resid_ref, full_ref)
    hidden_ref[rows_of(core), :] = mine_ref[...]

    def store(c, value):
        hidden_ref[rows_of(1 - core), c] = value

    gated(normed_ref, wg, wu, store)
    keep_ref[...] = down_slice(hidden_ref, wd, 2 * (1 - chip) + core)
    send_ref[...] = down_slice(hidden_ref, wd, 2 * (1 - chip) + 1 - core).astype(BF)


def home_kernel(hidden_ref, wd, own_ref, other_ref, keep_ref, send_ref):
    tp = place()[1]
    core, chip = tp % 2, tp // 2
    part = down_slice(hidden_ref, wd, 2 * chip + core)
    keep_ref[...] = part
    for i, ref in ((core, own_ref), (1 - core, other_ref)):
        keep_ref[rows_of(i), :] += ref[...]
    send_ref[...] = down_slice(hidden_ref, wd, 2 * chip + 1 - core).astype(BF)


def final_kernel(keep_ref, a_ref, b_ref, out_ref):
    out_ref[...] = (keep_ref[...] + a_ref[...].astype(F32) + b_ref[...].astype(F32)).astype(BF)


def sum_kernel(a_ref, b_ref, out_ref):
    out_ref[...] = (a_ref[...].astype(F32) + b_ref[...].astype(F32)).astype(BF)


def sds(shape, dtype=BF):
    return jax.ShapeDtypeStruct(shape, dtype)


def index_of(z, y, x):
    return z % 4 * 8 + y % 4 * 2 + x


GRID = [(z, y, x) for z in range(4) for y in range(4) for x in range(2)]
FLIP_X = [(index_of(z, y, x), index_of(z, y, 1 - x)) for z, y, x in GRID]
CORES = [(0, 1), (1, 0), (2, 3), (3, 2)]
CHIPS = [(0, 2), (2, 0), (1, 3), (3, 1)]


def along(second, k):
    out = []
    for z, y, x in GRID:
        for tp in range(4):
            if (tp % 2 == 0) != second:
                to = index_of(z + k, y, x)
            else:
                to = index_of(z, y + k, x)
            out.append((index_of(z, y, x) * 4 + tp, to * 4 + tp))
    return out


def stay(x):
    return pltpu.with_memory_space_constraint(x, pltpu.HBM)


def call(kernel, out, ins, outs, args, scratch=(), mib=56, flops=10**7, nbytes=MIB):
    return pl.pallas_call(
        kernel,
        out_shape=out,
        in_specs=ins,
        out_specs=outs,
        scratch_shapes=scratch,
        compiler_params=params(mib),
        cost_estimate=pl.CostEstimate(flops=flops, bytes_accessed=nbytes, transcendentals=0),
    )(*args)


def layer(tokens, order, gain_attn, gain_ffn, w_query, w_key, w_value, w_out, w_gate, w_up, w_down):
    rows, width = tokens.shape
    me, tp = place()
    every = ("blk", "tp")
    order = stay(order)
    table = jnp.asarray(angles())
    trig = sds((rows, 128), F32)
    half = sds((2 * HALF, 128))
    dma = pltpu.SemaphoreType.DMA

    normed, mine, send, cos, sin = call(
        kv_kernel,
        [sds((rows, width)), half, half, trig, trig],
        [SM, ANY, ANY, ANY, ANY, ANY], [VM] * 5,
        (order, stay(tokens), stay(gain_attn[None, :]), stay(w_key), stay(w_value), stay(table)),
        [
            pltpu.VMEM((2, 2 * HALF, 128), BF),
            pltpu.VMEM(tokens.shape, BF),
            pltpu.VMEM((1, width), F32),
            pltpu.VMEM((width, 256), BF),
            pltpu.VMEM(table.shape, F32),
            dma((10,)),
        ],
        mib=14,
    )
    got = lax.ppermute(send, "tp", CORES)
    one = call(pack_kernel, sds((2, 2 * HALF, 128)), [VM] * 2, VM, (mine[None], got[None]), mib=4)
    other = lax.ppermute(one, "blk", FLIP_X)
    two = call(
        pack_kernel, sds((2, 2, 2 * HALF, 128)), [VM] * 2, VM, (one[None], other[None]), mib=4
    )
    near = [lax.ppermute(two, every, along(False, k)) for k in COLUMNS[1:]]
    six = call(pack_kernel, sds((6, 2, 2 * HALF, 128)), [VM] * 3, VM, (two, *near), mib=8)
    column = lax.ppermute(near[1], every, along(False, 3))
    q = call(
        q_kernel, sds((2, 128, 1024)),
        [VM, ANY, VM, VM], VM,
        (normed, w_query, cos, sin),
        [pltpu.VMEM(w_query.shape, BF), dma((4,))],
        mib=16, flops=10**9, nbytes=4 * MIB,
    )
    q2 = lax.ppermute(q, "tp", CORES)
    wo2 = lax.ppermute(w_out, "tp", CORES)
    wx = lax.ppermute(w_out, "tp", CHIPS)
    wx2 = lax.ppermute(wx, "tp", CORES)
    far = {k: lax.ppermute(six, every, along(True, k)) for k in (3, 1)}
    side = {k: lax.ppermute(column, every, along(True, k)) for k in (3, 1)}
    far[2] = lax.ppermute(far[3], every, along(True, 3))
    side[2] = lax.ppermute(side[1], every, along(True, 1))
    side[0] = column

    state = [sds((4, 1, 1024), F32), sds((4, 80, 1024), F32)]
    m, acc = call(
        start_kernel, state, [SM] + [VM] * 3, [VM] * 2, (order, q, q2, six),
        mib=14, flops=2 * 10**9, nbytes=2 * MIB,
    )

    def add(kernel, parts, out, scratch=()):
        places = [((2,) if s is side else COLUMNS, k) for s, k in parts]
        return call(
            functools.partial(kernel, places), out,
            [SM] + [VM] * (4 + len(parts)), [VM] * 2,
            (order, q, q2, *[s[k] for s, k in parts], m, acc), scratch,
            mib=14, flops=2 * 10**9, nbytes=2 * MIB,
        )

    m, acc = add(next_kernel, [(far, 3)], state)
    m, acc = add(next_kernel, [(far, 1)], state)
    m, acc = add(next_kernel, [(side, 0), (side, 3), (side, 1)], state)
    keep, send = add(
        last_kernel, [(far, 2), (side, 2)], [sds((4, 80, 512), F32)] * 2,
        [pltpu.VMEM(s.shape, F32) for s in state],
    )
    got = lax.ppermute(send, "tp", CORES)
    heads = call(join_kernel, sds((HALF, 2 * w_out.shape[0])), [VM] * 2, VM, (keep, got), mib=8)
    there = lax.ppermute(heads, "tp", CHIPS)
    here = call(
        project_kernel, sds((HALF, width), F32), [VM] * 3, VM, (heads, w_out, wo2),
        mib=8, flops=10**9, nbytes=4 * MIB,
    )
    weights = (w_gate, w_up, w_down)
    weights = [pltpu.with_memory_space_constraint(w, pltpu.VMEM) for w in weights]
    share = width // lax.axis_size("tp")
    gain = gain_ffn[None, :]
    part = sds((HALF, width))
    slab = sds((rows, share))
    wide = sds((rows, share), F32)
    thin = sds((HALF, share), F32)
    att, normed, own = call(
        own_kernel, [part, part, thin], [VM] * 6, [VM] * 3,
        (here, there, wx, wx2, tokens, gain),
        [pltpu.VMEM((HALF, width), F32)], mib=8,
    )
    att = lax.ppermute(att, "tp", CORES)
    hidden = call(hidden_kernel, part, [VM] * 3, VM, (normed, *weights[:2]), mib=8, flops=2 * 10**9)
    other, hidden, keep, send = call(
        away_kernel, [thin, sds((rows, width)), wide, slab], [VM] * 7, [VM] * 4,
        (tokens, att, gain, hidden, *weights),
        [pltpu.VMEM((HALF, width), BF), pltpu.VMEM((HALF, width), F32)],
        mib=14, flops=4 * 10**9,
    )
    got = lax.ppermute(send, "tp", CORES)
    away = call(sum_kernel, slab, [VM] * 2, VM, (keep, got), mib=4)
    far_sum = lax.ppermute(away, "tp", CHIPS)
    keep, send = call(
        home_kernel, [wide, slab], [VM] * 4, [VM] * 2, (hidden, weights[2], own, other),
        mib=10, flops=10**9,
    )
    near_sum = lax.ppermute(send, "tp", CORES)
    return call(final_kernel, slab, [VM] * 3, VM, (keep, near_sum, far_sum), mib=8)


def solution(mesh):
    placed = (
        P("blk", None),
        P(),
        P(),
        P(),
        P(None, "tp"),
        P(None, "tp"),
        P(None, "tp"),
        P("tp", None),
        P(None, "tp"),
        P(None, "tp"),
        P("tp", None),
    )
    return jax.shard_map(
        layer, mesh=mesh, in_specs=placed, out_specs=P("blk", "tp"), check_vma=False
    )
```
